32 devices in a mesh: grp: 2 (over y), tgt: 4 (over z), src: 4 (over x, core).
Axes of the slice: x: 2, y: 2, z: 4, core: 2. Of those that a mesh axis runs over, the one named last changes fastest.
Arguments:
- target_rows: bfloat16 [2048, 4608], P(('grp', 'tgt', 'src')), parts along dimension 0, may hold values from -6 to 6
- target_pos: int32 [2048], P(('grp', 'tgt')), parts along dimension 0, may hold values from 0 to 255
- decoder_rows: bfloat16 [512, 4608], P(('grp', 'tgt', 'src')), parts along dimension 0, may hold values from -0.09375 to 0.09375
- source_pos: int32 [512], P('grp'), parts along dimension 0, may hold values from 0 to 255
- out_proj: bfloat16 [32, 4608, 128], P('src', 'tgt'), may hold values from -0.09375 to 0.09375
- value_proj: bfloat16 [16, 4608, 128], P('src'), may hold values from -1 to 1
- attention: bfloat16 [64, 256, 256], P(('grp', 'src'), 'tgt'), parts along dimension 0, may hold values from 0 to 1, as said below
- tile_pattern: int32 [8, 4], P('grp'), parts along dimension 0, may hold values from 0 to 1, as said below
Outputs:
- edges: bfloat16 [512, 1024], P(('grp', 'src'), 'tgt'), parts along dimension 0
The draws below stay inside these ranges and needn't reach their ends.
There are 2 independent parts, one for each index of `grp`. The reference program is written for one: setup_inputs(seed, part) draws one part's arguments, and reference() takes and returns one part's arrays. A program takes and returns all parts, laid end to end along the dimension named above; an argument that names none is the same for every part. Nothing has to cross between parts.
Inputs may be any that keep to these rules, and one draw needn't show every extreme that they name: Each row attention[h, p, :] is a probability distribution over the keys 0 to p: zero beyond p, summing to one. tile_pattern[b, c] is 1 where the tile of edges between source block b and target block c is kept, else 0.
All inputs are finite; a program needn't handle non-finite values.
Results may differ from the reference program's by a relative error of at most 0.0057.
Values may be sent and summed in bfloat16 or wider, within the bound.
A program may use at most 64 MiB of HBM per device.

```python
import jax
import jax.numpy as jnp
from jax import lax

D = 4608
H = 32
KV = 16
HD = 128
S = 256
TGT_DEV = 256
SRC_DEV = 64
BLOCKS = 4
NT = 1024
NS = 256


def draw_attention(key, part):
    noise_key = jax.random.fold_in(key, 11)
    logits = 3.0 * jax.random.normal(noise_key, (H, S, S), jnp.float32)
    query_pos = jnp.arange(S)[:, None]
    key_pos = jnp.arange(S)[None, :]
    causal = key_pos <= query_pos
    logits = jnp.where(causal[None], logits, -1e+30)
    weights = jax.nn.softmax(logits, axis=-1)
    return weights.astype(jnp.bfloat16)


def draw_tile_pattern(key, part):
    level_key, roll_key = jax.random.split(jax.random.fold_in(key, 23))
    levels = jnp.array([6, 12, 25, 50, 100], jnp.int32)
    choose = jax.random.randint(level_key, (BLOCKS,), 0, 5)
    dice_rolls = jax.random.randint(roll_key, (BLOCKS, BLOCKS), 0, 100)
    return (dice_rolls < levels[choose][None, :]).astype(jnp.int32)


def touch_ends(entries, rng, smallest, top_value):
    longest = entries.shape.index(max(entries.shape))
    spots = []
    for shift in (0, 1):
        where = [jax.random.randint(jax.random.fold_in(rng, axis), (), 0, length) for axis, length in enumerate(entries.shape)]
        where[longest] = (where[longest] + shift) % entries.shape[longest]
        spots.append(tuple(where))
    return entries.at[spots[0]].set(smallest).at[spots[1]].set(top_value)


def block_levels(key, shape, cuts, low, high):
    level = 1.0
    for position, shards_of in cuts:
        steps = jax.random.uniform(jax.random.fold_in(jax.random.fold_in(key, 6), position), (shards_of,), jnp.float32, low / len(cuts), high / len(cuts))
        level = level * jnp.repeat(jnp.exp(steps), shape[position] // shards_of).reshape((-1,) + (1,) * (len(shape) - 1 - position))
    return level


def centred(stream_key, shape, deviation, most, pieces=(), held_as=jnp.bfloat16):
    result = deviation * jax.random.normal(stream_key, shape, jnp.float32)
    if pieces:
        result = result * block_levels(stream_key, shape, pieces, -0.22, 0.18)
    return jnp.clip(result, -most, most).astype(held_as)


def setup_inputs(seed: int = 0, part: int = 0) -> dict:
    key_of = jax.random.split(jax.random.key(seed), 9)
    part_keys = jax.random.split(jax.random.fold_in(key_of[8], part), 9)
    return {
        "target_rows": centred(part_keys[0], (NT, D), 1.0, 6.0, ((0, 16),)),
        "target_pos": touch_ends(jax.random.randint(part_keys[1], (NT,), 0, S), jax.random.fold_in(part_keys[1], 1), 0, S - 1).astype(jnp.int32),
        "decoder_rows": centred(part_keys[2], (NS, D), D ** -0.5, 0.09375, ((0, 16),)),
        "source_pos": touch_ends(jax.random.randint(part_keys[3], (NS,), 0, S), jax.random.fold_in(part_keys[3], 1), 0, S - 1).astype(jnp.int32),
        "out_proj": centred(key_of[4], (H, D, HD), D ** -0.5, 0.09375, ((0, 4), (1, 4))),
        "value_proj": centred(key_of[5], (KV, D, HD), (HD // 4) ** -0.5, 1.0, ((0, 4),)),
        "attention": draw_attention(jax.random.fold_in(jax.random.fold_in(key_of[8], part), 71), part),
        "tile_pattern": draw_tile_pattern(jax.random.fold_in(jax.random.fold_in(key_of[8], part), 71), part),
    }


def reference(target_rows, target_pos, decoder_rows, source_pos, out_proj, value_proj, attention, tile_pattern):
    highest = lax.Precision.HIGHEST
    targets_wide = target_rows.astype(jnp.float32)
    sources_wide = decoder_rows.astype(jnp.float32)
    head_reads = jnp.einsum('td,hde->the', targets_wide, out_proj.astype(jnp.float32), precision=highest).astype(jnp.bfloat16)
    source_values = jnp.einsum('nd,gde->nge', sources_wide, value_proj.astype(jnp.float32), precision=highest).astype(jnp.bfloat16)
    same_place = (source_pos[:, None] == target_pos[None, :]).astype(jnp.float32)
    direct = jnp.dot(sources_wide, targets_wide.T, precision=highest) * same_place
    repeat = H // KV

    def add_head(head_index, running):
        group_index = head_index // repeat
        value_part = lax.dynamic_index_in_dim(source_values, group_index, 1, keepdims=False).astype(jnp.float32)
        read_part = lax.dynamic_index_in_dim(head_reads, head_index, 1, keepdims=False).astype(jnp.float32)
        scores = jnp.dot(value_part, read_part.T, precision=highest)
        attn_table = lax.dynamic_index_in_dim(attention, head_index, 0, keepdims=False).astype(jnp.float32)
        weights = jnp.take(jnp.take(attn_table, target_pos, axis=0), source_pos, axis=1).T
        return running + weights * scores

    mixed_term = lax.fori_loop(0, H, add_head, jnp.zeros((NS, NT), jnp.float32))
    keep_mask = jnp.repeat(jnp.repeat(tile_pattern, SRC_DEV, axis=0), TGT_DEV, axis=1).astype(jnp.float32)
    return (keep_mask * (direct + mixed_term)).astype(jnp.bfloat16)
```

```python
import functools

import jax
import jax.numpy as jnp
from jax import lax
from jax.experimental import pallas as pl
from jax.experimental.pallas import tpu as pltpu
from jax.sharding import PartitionSpec as P


def passed_along(value, axis, steps):
    count = lax.axis_size(axis)
    pairs = [(source, (source + steps) % count) for source in range(count)]
    return lax.ppermute(value, axis, pairs)


def gathered_shards(
    target_rows, target_pos, decoder_rows, source_pos, out_proj, value_proj, attention, tile_pattern
):
    blocks = lax.axis_size("tgt")
    column = lax.axis_index("tgt")
    src_lane = lax.axis_index("src")
    full_targets, full_sources = (
        lax.all_gather(target_rows, "src", axis=0, tiled=True),
        lax.all_gather(decoder_rows, "src", axis=0, tiled=True),
    )
    tgt_dev = full_targets.shape[0]
    src_dev = full_sources.shape[0]
    sub_rows = decoder_rows.shape[0]
    heads_here = out_proj.shape[0]
    head_dim = out_proj.shape[2]
    groups_here = value_proj.shape[0]
    repeat = heads_here // groups_here
    read_sum = jnp.einsum(
        "td,hde->the",
        full_targets,
        lax.all_gather(out_proj, "tgt", axis=1, tiled=True),
        preferred_element_type=jnp.float32,
    )
    head_reads = read_sum.astype(jnp.bfloat16).reshape(tgt_dev, groups_here, repeat, head_dim)
    values = jnp.einsum("sd,gde->sge", full_sources, value_proj, preferred_element_type=jnp.float32)
    values = values.astype(jnp.bfloat16).reshape(src_dev, groups_here * head_dim)
    attn_table = lax.all_gather(attention, "tgt", axis=1, tiled=True)
    target_attn = jnp.take(attn_table, target_pos, axis=1)
    keyed_attn = jnp.transpose(target_attn, (0, 2, 1))

    def edge_tile(payload, block_index):
        decoder_part, value_part = payload
        key_positions = lax.dynamic_slice_in_dim(source_pos, block_index * src_dev, src_dev)
        weights = jnp.take(keyed_attn, key_positions, axis=1).astype(jnp.float32)
        scores = jnp.einsum(
            "sgd,tgrd->grst",
            value_part.reshape(src_dev, groups_here, head_dim),
            head_reads,
            preferred_element_type=jnp.float32,
        )
        scores = scores.reshape(heads_here, src_dev, tgt_dev)
        mixed_term = jnp.sum(weights * scores, axis=0)
        own_positions = lax.dynamic_slice_in_dim(key_positions, src_lane * sub_rows, sub_rows)
        same_place = (own_positions[:, None] == target_pos[None, :]).astype(jnp.float32)
        direct = (
            jnp.einsum("sd,td->st", decoder_part, full_targets, preferred_element_type=jnp.float32)
            * same_place
        )
        own_rows = lax.dynamic_slice_in_dim(mixed_term, src_lane * sub_rows, sub_rows, 0)
        return lax.dynamic_update_slice_in_dim(
            mixed_term, own_rows + direct, src_lane * sub_rows, 0
        )

    def place_tile(partial_value, payload, block_index):
        kept_flag = tile_pattern[block_index, column]
        piece_tile = edge_tile(payload, block_index) * kept_flag.astype(jnp.float32)
        return lax.dynamic_update_slice_in_dim(partial_value, piece_tile, block_index * src_dev, 0)

    own_block = (decoder_rows, values)
    partial_value = jnp.zeros((blocks * src_dev, tgt_dev), jnp.float32)
    partial_value = place_tile(partial_value, own_block, column)

    def cycle_turn(turn_index, state_carry):
        forward_block, backward_block, running = state_carry
        forward_block = passed_along((forward_block[0], forward_block[1]), "tgt", 1)
        backward_block = passed_along((backward_block[0], backward_block[1]), "tgt", -1)
        running = place_tile(running, forward_block, (column - turn_index) % blocks)
        running = place_tile(running, backward_block, (column + turn_index) % blocks)
        return (forward_block, backward_block, running)

    forward_block, backward_block, partial_value = lax.fori_loop(
        1, blocks // 2, cycle_turn, (own_block, own_block, partial_value)
    )
    forward_block = passed_along((forward_block[0], forward_block[1]), "tgt", 1)
    partial_value = place_tile(partial_value, forward_block, (column - blocks // 2) % blocks)
    summed = lax.psum_scatter(partial_value, "src", scatter_dimension=0, tiled=True)
    return summed.astype(jnp.bfloat16)


F32 = jnp.float32
BF16 = jnp.bfloat16
MESH = pl.DeviceIdType.MESH


def dot(a, b):
    return jnp.dot(a, b, preferred_element_type=F32)


def dot_nt(a, b):
    return lax.dot_general(a, b, (((1,), (1,)), ((), ())), preferred_element_type=F32)


def edge_kernel(
    nt, ns, tgt_hbm, tpos_hbm, dec_hbm, srow_hbm, oproj_hbm, vproj_hbm, attn_hbm, pat_ref,
    out_ref,
    oproj, vproj, tslices, dslices, decfull, attn, tpos, srow, values, reads, pick, attn_n, onehot,
    edges, core_in, x_out, x_in, z_out, z_in, scol_ref,
    local_sem, zt_s, zt_r, zd_s, zd_r, zp_s, zp_r, ar_s, al_s, a_r, vr_s, vl_s, v_r,
    xt_s, xt_r, ct_s, ct_r, xf_s, xf_r, cf_s, cf_r, ce_s, ce_r, xe_s, xe_r, ze_s, ze_r,
):
    c = lax.axis_index("tgt")
    s = lax.axis_index("src")
    nx = ns // 2
    x = s // 2
    core = s % 2
    mate = x * 2 + 1 - core
    rows, depth = tslices.shape[1] // ns, tslices.shape[2]
    sub = dec_hbm.shape[0]
    heads = oproj.shape[0]
    groups = vproj.shape[0]
    repeat = heads // groups
    block = sub * ns
    queries, keys = attn_hbm.shape[1:]
    targets = tpos.shape[2]
    total = scol_ref.shape[0]
    own = edges.shape[1] // ns
    hd = vproj.shape[2]

    inner = (c > 0) & (c + 1 < nt)

    def table(rank):
        rows_of = [[i] + sorted((b for b in range(nt) if b != i), key=lambda b: rank(i, b)) for i in range(nt)]

        def entry(j):
            b = rows_of[0][j]
            for i in range(1, nt):
                b = jnp.where(c == i, rows_of[i][j], b)
            return b

        return [entry(j) for j in range(nt)]

    def sent_rank(i, b):
        return abs(b - i) if 0 < i < nt - 1 else -abs(b - i)

    def got_rank(i, b):
        far = abs(b - i)
        return (-far, b in (0, nt - 1)) if 0 < i < nt - 1 else (b in (0, nt - 1) and -far, far)

    targets_of = table(sent_rank)
    order = table(got_rank)
    last_of = table(lambda i, b: -b)

    def xsrc(dx):
        return lax.rem(x + dx, nx) * 2 + core

    pending = []

    def remote(src, dst, ssem, rsem, axis, index):
        return pltpu.make_async_remote_copy(
            src_ref=src, dst_ref=dst, send_sem=ssem, recv_sem=rsem,
            device_id={axis: index}, device_id_type=MESH,
        )

    def send(src, dst, ssem, rsem, axis, index):
        remote(src, dst, ssem, rsem, axis, index).start()
        pending.append((None, lambda: remote(src, dst, ssem, rsem, axis, index)))

    def arrived(dst, rsem):
        remote(dst, dst, local_sem.at[0], rsem, "src", mate).wait_recv()

    barrier = pltpu.get_barrier_semaphore()
    for j in range(1, nt):
        pl.semaphore_signal(barrier, inc=1, device_id={"tgt": order[j]}, device_id_type=MESH)
    for dx in range(1, nx):
        pl.semaphore_signal(barrier, inc=1, device_id={"src": xsrc(dx)}, device_id_type=MESH)
    pl.semaphore_signal(barrier, inc=1, device_id={"src": mate}, device_id_type=MESH)

    def cols(b):
        return pl.ds(pl.multiple_of(b * depth, 128), depth)

    def trow(lane):
        return pl.ds(pl.multiple_of(lane * rows, rows), rows)

    def drow(lane):
        return pl.ds(pl.multiple_of(lane * sub, sub), sub)

    def qrow(b):
        return pl.ds(pl.multiple_of(b * queries, queries), queries)

    def vrow(b):
        return pl.ds(pl.multiple_of(b * block, block), block)

    def erow(lane):
        return pl.ds(pl.multiple_of(lane * own, own), own)

    fetch = [
        pltpu.make_async_copy(dec_hbm, decfull.at[drow(s)], local_sem.at[1]),
        pltpu.make_async_copy(srow_hbm, srow, local_sem.at[2]),
        pltpu.make_async_copy(tpos_hbm, tpos.at[c], local_sem.at[3]),
        pltpu.make_async_copy(vproj_hbm, vproj, local_sem.at[4]),
        pltpu.make_async_copy(tgt_hbm.at[:, cols(c)], tslices.at[c, trow(s)], local_sem.at[5]),
        pltpu.make_async_copy(dec_hbm.at[:, cols(c)], dslices.at[drow(c)], local_sem.at[6]),
        pltpu.make_async_copy(oproj_hbm, oproj, local_sem.at[7]),
        pltpu.make_async_copy(attn_hbm, attn.at[:, qrow(c), :], local_sem.at[8]),
    ]
    for cp in fetch[:7]:
        cp.start()
    pl.semaphore_wait(barrier, nt - 1 + nx)

    half = keys // 2
    lowest = half // queries if half % 128 == 0 else 0

    def attn_copy(b, g, ssem, device, act, src=None):
        part = pl.ds(g * repeat, repeat)

        def view(lanes):
            dst = attn.at[part, qrow(b), lanes]
            return dst if src is None else src.at[part, :, lanes], dst

        @pl.when(b < lowest)
        def _():
            a, d = view(pl.ds(0, half))
            act(remote(a, d, ssem.at[b, g], a_r.at[b, g], "tgt", device))

        @pl.when(b >= lowest)
        def _():
            a, d = view(pl.ds(0, keys))
            act(remote(a, d, ssem.at[b, g], a_r.at[b, g], "tgt", device))

    def value_copy(b, ssem, device):
        dst = values.at[:, vrow(b), :]
        return remote(dst, dst, ssem.at[b], v_r.at[b], "tgt", device)

    start = lambda copy: copy.start()
    wait_send = lambda copy: copy.wait_send()
    wait_recv = lambda copy: copy.wait_recv()

    def rightward(act):
        pl.when(c + 1 < nt)(act)

    def leftward(act):
        pl.when(c > 0)(act)

    for dx in range(1, nx):
        send(dec_hbm, decfull.at[drow(s)], xf_s.at[dx], xf_r.at[x], "src", xsrc(dx))
    send(dec_hbm, decfull.at[drow(s)], cf_s.at[x], cf_r.at[x], "src", mate)
    def spread_copies(b):
        return (
            remote(tgt_hbm.at[:, cols(b)], tslices.at[c, trow(s)], zt_s.at[b], zt_r.at[c], "tgt", b),
            remote(dec_hbm.at[:, cols(b)], dslices.at[drow(c)], zd_s.at[b], zd_r.at[c], "tgt", b),
            remote(tpos_hbm, tpos.at[c], zp_s.at[b], zp_r.at[c], "tgt", b),
        )

    def spread(j):
        b = targets_of[j]
        for copy in spread_copies(b):
            copy.start()

    spread(1)
    spread(2)
    for dx in range(1, nx):
        send(tgt_hbm.at[:, cols(c)], tslices.at[c, trow(s)], xt_s.at[c, dx], xt_r.at[c, x], "src", xsrc(dx))
    send(tgt_hbm.at[:, cols(c)], tslices.at[c, trow(s)], ct_s.at[c, x], ct_r.at[c, x], "src", mate)

    fetch[1].wait()
    fetch[2].wait()
    scol_ref[...] = jnp.transpose(jnp.broadcast_to(srow[...], (128, total)))[:, :1]
    pick[...] = (scol_ref[...] == lax.broadcasted_iota(jnp.int32, (total, keys), 1)).astype(BF16)
    for b in range(lowest):
        attn[:, b * queries:(b + 1) * queries, half:] = jnp.zeros((heads, queries, keys - half), BF16)
    fetch[7].start()

    def relay(k, copy_in, copy_on):
        @pl.when(c - k >= 0)
        def _():
            copy_in(c - k)
            rightward(lambda: copy_on(c - k, 0))

        @pl.when(c + k < nt)
        def _():
            copy_in(c + k)
            leftward(lambda: copy_on(c + k, 1))

    def attn_step(k, g):
        relay(
            k, lambda b: attn_copy(b, g, ar_s, c, wait_recv),
            lambda b, left: attn_copy(b, g, al_s if left else ar_s, c - 1 if left else c + 1, start),
        )

    def value_step(k):
        relay(
            k, lambda b: value_copy(b, vr_s, c).wait_recv(),
            lambda b, left: value_copy(b, vl_s if left else vr_s, c - 1 if left else c + 1).start(),
        )

    def take(j):
        b = order[j]
        arrived(tslices.at[b, trow(s)], zt_r.at[b])
        for dx in range(1, nx):
            send(tslices.at[b, trow(s)], tslices.at[b, trow(s)], xt_s.at[b, dx], xt_r.at[b, x], "src", xsrc(dx))
        send(tslices.at[b, trow(s)], tslices.at[b, trow(s)], ct_s.at[b, x], ct_r.at[b, x], "src", mate)

    fetch[0].wait()
    for dx in range(1, nx):
        z = lax.rem(x + dx, nx)
        y = xsrc(dx)
        arrived(decfull.at[drow(y)], xf_r.at[z])
        send(decfull.at[drow(y)], decfull.at[drow(y)], cf_s.at[z], cf_r.at[z], "src", mate)
    for dx in range(nx):
        z = lax.rem(x + dx, nx)
        arrived(decfull.at[drow(z * 2 + 1 - core)], cf_r.at[z])
    fetch[3].wait()

    @pl.loop(0, groups)
    def _(g):
        values[g, vrow(c)] = dot(decfull[...], vproj[g]).astype(BF16)

    fetch[7].wait()
    rightward(lambda: value_copy(c, vr_s, c + 1).start())
    leftward(lambda: value_copy(c, vl_s, c - 1).start())
    for j in range(3, nt):
        spread(j)
    rightward(lambda: attn_copy(c, 0, ar_s, c + 1, start, attn_hbm))
    leftward(lambda: attn_copy(c, 0, al_s, c - 1, start, attn_hbm))
    rightward(lambda: attn_copy(c, 1, ar_s, c + 1, start, attn_hbm))
    leftward(lambda: attn_copy(c, 1, al_s, c - 1, start, attn_hbm))
    rightward(lambda: attn_copy(c, 2, ar_s, c + 1, start, attn_hbm))
    leftward(lambda: attn_copy(c, 2, al_s, c - 1, start, attn_hbm))
    rightward(lambda: attn_copy(c, 3, ar_s, c + 1, start, attn_hbm))
    leftward(lambda: attn_copy(c, 3, al_s, c - 1, start, attn_hbm))

    def cross(j):
        b = order[j]
        for dx in range(1, nx):
            z = lax.rem(x + dx, nx)
            y = z * 2 + core
            arrived(tslices.at[b, trow(y)], xt_r.at[b, z])
            send(tslices.at[b, trow(y)], tslices.at[b, trow(y)], ct_s.at[b, z], ct_r.at[b, z], "src", mate)

    def ready(j):
        b = order[j]
        if j == 0:
            fetch[4].wait()
            fetch[5].wait()
            fetch[6].wait()
        else:
            arrived(dslices.at[drow(b)], zd_r.at[b])
            arrived(tpos.at[b], zp_r.at[b])
        for dx in range(nx):
            z = lax.rem(x + dx, nx)
            arrived(tslices.at[b, trow(z * 2 + 1 - core)], ct_r.at[b, z])

    def read_block(j):
        b = order[j]

        @pl.loop(0, groups)
        def _(g):
            pair = jnp.concatenate([oproj[g * repeat + r] for r in range(repeat)], axis=1)
            reads[b, g] = dot(tslices[b], pair).astype(BF16)
        onehot[b] = (
            lax.broadcasted_iota(jnp.int32, (nt * queries, targets), 0) == tpos[b]
        ).astype(BF16)

    def start_edges(j):
        b = order[j]
        direct = dot_nt(dslices[...], tslices[b])
        here = tpos[b]
        edges[b] = jnp.zeros(edges.shape[1:], F32)
        for p in range(nt):
            at = pl.ds(pl.multiple_of(p * block + s * sub, sub), sub)
            same = (scol_ref[at] == here).astype(F32)
            edges[b, at] = direct[p * sub:(p + 1) * sub] * same

    def pick_keys(g):
        for r in range(repeat):
            attn_n[g * repeat + r] = dot_nt(pick[...], attn[g * repeat + r]).astype(BF16)

    def mix(g, b):
        terms = None
        for r in range(repeat):
            term = dot(attn_n[g * repeat + r], onehot[b]) * dot_nt(values[g], reads[b, g, :, r * hd:(r + 1) * hd])
            terms = term if terms is None else terms + term
        edges[b] += terms

    def to_mate(b):
        for z in range(nx):
            send(edges.at[b, erow(z * 2 + 1 - core)], core_in.at[b, z], ce_s.at[b, z], ce_r.at[b, z], "src", mate)

    def over_x(b):
        for dx in range(1, nx):
            z = lax.rem(x + dx, nx)
            arrived(core_in.at[b, z], ce_r.at[b, z])
            x_out[b, z] = (edges[b, erow(z * 2 + core)] + core_in[b, z]).astype(BF16)
            send(x_out.at[b, z], x_in.at[b, x], xe_s.at[b, z], xe_r.at[b, x], "src", z * 2 + core)
        arrived(core_in.at[b, x], ce_r.at[b, x])

    def over_z(b, away):
        mine = edges[b, erow(s)] + core_in[b, x]
        for dx in range(1, nx):
            z = lax.rem(x + dx, nx)
            arrived(x_in.at[b, z], xe_r.at[b, z])
            mine += x_in[b, z].astype(F32)
        if away:
            z_out[b] = mine.astype(BF16)
            send(z_out.at[b], z_in.at[c], ze_s.at[b], ze_r.at[c], "tgt", b)
        return mine

    take(1)
    cross(0)
    ready(0)
    read_block(0)
    take(2)
    cross(1)
    take(3)
    value_step(1)
    ready(1)
    read_block(1)
    cross(2)
    attn_step(1, 0)
    ready(2)
    read_block(2)
    attn_step(1, 1)
    cross(3)
    attn_step(1, 2)
    ready(3)
    read_block(3)
    attn_step(1, 3)
    start_edges(0)
    value_step(2)
    attn_step(2, 0)
    start_edges(1)
    start_edges(2)
    start_edges(3)
    value_step(3)
    for g in range(groups):
        for k in range(1, nt):
            if (k, g) not in [(1, 0), (1, 1), (1, 2), (1, 3), (2, 0)]:
                attn_step(k, g)
        pick_keys(g)
        for j in list(range(1, nt)) + [0]:
            mix(g, last_of[j])
            if g == groups - 1:
                to_mate(last_of[j])
    for j in list(range(1, nt)) + [0]:
        over_x(last_of[j])
    for j in range(1, nt):
        over_z(last_of[j], True)
    mine = over_z(c, False)
    for j in range(1, nt):
        for copy in spread_copies(order[j]):
            copy.wait_send()
    for _, again in pending:
        again().wait_send()
    for k in range(nt):
        @pl.when((c - k >= 0) & (c + 1 < nt))
        def _():
            for g in range(groups):
                attn_copy(c - k, g, ar_s, c + 1, wait_send)
            value_copy(c - k, vr_s, c + 1).wait_send()

        @pl.when((c + k < nt) & (c > 0))
        def _():
            for g in range(groups):
                attn_copy(c + k, g, al_s, c - 1, wait_send)
            value_copy(c + k, vl_s, c - 1).wait_send()

    for j in range(1, nt):
        b = order[j]
        arrived(z_in.at[b], ze_r.at[b])
        mine += z_in[b].astype(F32)
    kept = pat_ref[(s * own) // block, c]
    out_ref[...] = (mine * kept.astype(F32)).astype(BF16)


def resident_shards(
    target_rows, target_pos, decoder_rows, source_pos, out_proj, value_proj, attention, tile_pattern
):
    nt, ns = lax.axis_size("tgt"), lax.axis_size("src")
    rows = target_rows.shape[0]
    sub, width = decoder_rows.shape
    heads, depth, head_dim = out_proj.shape
    groups = value_proj.shape[0]
    repeat = heads // groups
    _, queries, keys = attention.shape
    total = source_pos.shape[0]
    targets = target_pos.shape[0]
    own = total // ns
    nx = ns // 2
    vmem = pl.BlockSpec(memory_space=pltpu.VMEM)
    hbm = pl.BlockSpec(memory_space=pl.ANY)
    sem = lambda *shape: pltpu.SemaphoreType.DMA(shape)
    return pl.pallas_call(
        functools.partial(edge_kernel, nt, ns),
        out_shape=jax.ShapeDtypeStruct((own, targets), BF16),
        in_specs=[hbm, hbm, hbm, hbm, hbm, hbm, hbm, pl.BlockSpec(memory_space=pltpu.SMEM)],
        out_specs=vmem,
        scratch_shapes=[
            pltpu.VMEM(out_proj.shape, BF16),
            pltpu.VMEM(value_proj.shape, BF16),
            pltpu.VMEM((nt, ns * rows, depth), BF16),
            pltpu.VMEM((nt * sub, depth), BF16),
            pltpu.VMEM((ns * sub, width), BF16),
            pltpu.VMEM((heads, nt * queries, keys), BF16),
            pltpu.VMEM((nt, 1, targets), jnp.int32),
            pltpu.VMEM((1, total), jnp.int32),
            pltpu.VMEM((groups, total, head_dim), BF16),
            pltpu.VMEM((nt, groups, targets, repeat * head_dim), BF16),
            pltpu.VMEM((total, keys), BF16),
            pltpu.VMEM((heads, total, nt * queries), BF16),
            pltpu.VMEM((nt, nt * queries, targets), BF16),
            pltpu.VMEM((nt, total, targets), F32),
            pltpu.VMEM((nt, nx, own, targets), F32),
            pltpu.VMEM((nt, nx, own, targets), BF16),
            pltpu.VMEM((nt, nx, own, targets), BF16),
            pltpu.VMEM((nt, own, targets), BF16),
            pltpu.VMEM((nt, own, targets), BF16),
            pltpu.VMEM((total, 1), jnp.int32),
            sem(9),
            sem(nt), sem(nt), sem(nt), sem(nt), sem(nt), sem(nt),
            sem(nt, groups), sem(nt, groups), sem(nt, groups), sem(nt), sem(nt), sem(nt),
            sem(nt, nx), sem(nt, nx), sem(nt, nx), sem(nt, nx),
            sem(nx), sem(nx), sem(nx), sem(nx),
            sem(nt, nx), sem(nt, nx), sem(nt, nx), sem(nt, nx), sem(nt), sem(nt),
        ],
        compiler_params=pltpu.CompilerParams(
            collective_id=0, has_side_effects=True, vmem_limit_bytes=60 * 1024 * 1024
        ),
    )(
        target_rows, target_pos.reshape(1, targets), decoder_rows, source_pos.reshape(1, total),
        out_proj, value_proj, attention, tile_pattern,
    )


def resident_bytes(nt, ns, width, heads, depth, groups, rows, total, targets):
    weights = heads * depth * 128 + groups * width * 128
    gathered = nt * ns * rows * depth + nt * heads * targets * 128
    return 2 * (weights + gathered) + 4 * nt * total * targets * 2


def shards(
    target_rows, target_pos, decoder_rows, source_pos, out_proj, value_proj, attention, tile_pattern
):
    nt, ns = lax.axis_size("tgt"), lax.axis_size("src")
    heads, depth, head_dim = out_proj.shape
    need = resident_bytes(
        nt, ns, target_rows.shape[1], heads, depth, value_proj.shape[0], target_rows.shape[0],
        source_pos.shape[0], target_pos.shape[0],
    )
    fits = (
        depth % 128 == 0 and head_dim == 128 and ns % 2 == 0 and nt > 2
        and decoder_rows.shape[0] % 16 == 0 and attention.shape[1] % 16 == 0
        and need < 40 * 1024 * 1024
    )
    plan = resident_shards if fits else gathered_shards
    return plan(
        target_rows, target_pos, decoder_rows, source_pos, out_proj, value_proj, attention, tile_pattern
    )


def solution(mesh):
    return jax.shard_map(
        shards,
        mesh=mesh,
        in_specs=(
            P(("grp", "tgt", "src"), None),
            P(("grp", "tgt")),
            P(("grp", "tgt", "src"), None),
            P("grp"),
            P("src", "tgt", None),
            P("src", None, None),
            P(("grp", "src"), "tgt", None),
            P("grp", None),
        ),
        out_specs=P(("grp", "src"), "tgt"),
        check_vma=False,
    )
```

```python
import functools

import jax
import jax.numpy as jnp
from jax import lax
from jax.experimental import pallas as pl
from jax.experimental.pallas import tpu as pltpu
from jax.sharding import PartitionSpec as P


def passed_along(value, axis, steps):
    count = lax.axis_size(axis)
    pairs = [(source, (source + steps) % count) for source in range(count)]
    return lax.ppermute(value, axis, pairs)


def gathered_shards(
    target_rows, target_pos, decoder_rows, source_pos, out_proj, value_proj, attention, tile_pattern
):
    blocks = lax.axis_size("tgt")
    column = lax.axis_index("tgt")
    src_lane = lax.axis_index("src")
    full_targets, full_sources = (
        lax.all_gather(target_rows, "src", axis=0, tiled=True),
        lax.all_gather(decoder_rows, "src", axis=0, tiled=True),
    )
    tgt_dev = full_targets.shape[0]
    src_dev = full_sources.shape[0]
    sub_rows = decoder_rows.shape[0]
    heads_here = out_proj.shape[0]
    head_dim = out_proj.shape[2]
    groups_here = value_proj.shape[0]
    repeat = heads_here // groups_here
    read_sum = jnp.einsum(
        "td,hde->the",
        full_targets,
        lax.all_gather(out_proj, "tgt", axis=1, tiled=True),
        preferred_element_type=jnp.float32,
    )
    head_reads = read_sum.astype(jnp.bfloat16).reshape(tgt_dev, groups_here, repeat, head_dim)
    values = jnp.einsum("sd,gde->sge", full_sources, value_proj, preferred_element_type=jnp.float32)
    values = values.astype(jnp.bfloat16).reshape(src_dev, groups_here * head_dim)
    attn_table = lax.all_gather(attention, "tgt", axis=1, tiled=True)
    target_attn = jnp.take(attn_table, target_pos, axis=1)
    keyed_attn = jnp.transpose(target_attn, (0, 2, 1))

    def edge_tile(payload, block_index):
        decoder_part, value_part = payload
        key_positions = lax.dynamic_slice_in_dim(source_pos, block_index * src_dev, src_dev)
        weights = jnp.take(keyed_attn, key_positions, axis=1).astype(jnp.float32)
        scores = jnp.einsum(
            "sgd,tgrd->grst",
            value_part.reshape(src_dev, groups_here, head_dim),
            head_reads,
            preferred_element_type=jnp.float32,
        )
        scores = scores.reshape(heads_here, src_dev, tgt_dev)
        mixed_term = jnp.sum(weights * scores, axis=0)
        own_positions = lax.dynamic_slice_in_dim(key_positions, src_lane * sub_rows, sub_rows)
        same_place = (own_positions[:, None] == target_pos[None, :]).astype(jnp.float32)
        direct = (
            jnp.einsum("sd,td->st", decoder_part, full_targets, preferred_element_type=jnp.float32)
            * same_place
        )
        own_rows = lax.dynamic_slice_in_dim(mixed_term, src_lane * sub_rows, sub_rows, 0)
        return lax.dynamic_update_slice_in_dim(
            mixed_term, own_rows + direct, src_lane * sub_rows, 0
        )

    def place_tile(partial_value, payload, block_index):
        kept_flag = tile_pattern[block_index, column]
        piece_tile = edge_tile(payload, block_index) * kept_flag.astype(jnp.float32)
        return lax.dynamic_update_slice_in_dim(partial_value, piece_tile, block_index * src_dev, 0)

    own_block = (decoder_rows, values)
    partial_value = jnp.zeros((blocks * src_dev, tgt_dev), jnp.float32)
    partial_value = place_tile(partial_value, own_block, column)

    def cycle_turn(turn_index, state_carry):
        forward_block, backward_block, running = state_carry
        forward_block = passed_along((forward_block[0], forward_block[1]), "tgt", 1)
        backward_block = passed_along((backward_block[0], backward_block[1]), "tgt", -1)
        running = place_tile(running, forward_block, (column - turn_index) % blocks)
        running = place_tile(running, backward_block, (column + turn_index) % blocks)
        return (forward_block, backward_block, running)

    forward_block, backward_block, partial_value = lax.fori_loop(
        1, blocks // 2, cycle_turn, (own_block, own_block, partial_value)
    )
    forward_block = passed_along((forward_block[0], forward_block[1]), "tgt", 1)
    partial_value = place_tile(partial_value, forward_block, (column - blocks // 2) % blocks)
    summed = lax.psum_scatter(partial_value, "src", scatter_dimension=0, tiled=True)
    return summed.astype(jnp.bfloat16)


F32 = jnp.float32
BF16 = jnp.bfloat16
MESH = pl.DeviceIdType.MESH


def dot(a, b):
    return jnp.dot(a, b, preferred_element_type=F32)


def dot_nt(a, b):
    return lax.dot_general(a, b, (((1,), (1,)), ((), ())), preferred_element_type=F32)


def edge_kernel(
    nt, ns, tgt_hbm, tpos_hbm, dec_hbm, srow_hbm, oproj_hbm, vproj_hbm, attn_hbm, pat_hbm,
    out_ref,
    oproj, vproj, tslices, dslices, decfull, attn, packs, tpos, srow, values, reads, pick, attn_n, onehot,
    edges, core_in, x_out, x_in, z_out, z_in, scol_ref, pat_ref,
    local_sem, zt_s, zt_r, zd_s, zd_r, zp_s, zp_r, ar_s, al_s, a_r, vr_s, vl_s, v_r,
    xt_s, xt_r, ct_s, ct_r, xf_s, xf_r, cf_s, cf_r, ce_s, ce_r, xe_s, xe_r, ze_s, ze_r,
):
    c = lax.axis_index("tgt")
    s = lax.axis_index("src")
    nx = ns // 2
    x = s // 2
    core = s % 2
    mate = x * 2 + 1 - core
    rows, depth = tslices.shape[1] // ns, tslices.shape[2]
    sub = dec_hbm.shape[0]
    heads = oproj.shape[0]
    groups = vproj.shape[0]
    repeat = heads // groups
    block = sub * ns
    queries, keys = attn_hbm.shape[1:]
    targets = tpos.shape[2]
    total = scol_ref.shape[0]
    own = edges.shape[1] // ns
    hd = vproj.shape[2]

    inner = (c > 0) & (c + 1 < nt)

    def table(rank):
        rows_of = [[i] + sorted((b for b in range(nt) if b != i), key=lambda b: rank(i, b)) for i in range(nt)]

        def entry(j):
            b = rows_of[0][j]
            for i in range(1, nt):
                b = jnp.where(c == i, rows_of[i][j], b)
            return b

        return [entry(j) for j in range(nt)]

    def sent_rank(i, b):
        return abs(b - i) if 0 < i < nt - 1 else -abs(b - i)

    def got_rank(i, b):
        far = abs(b - i)
        return (-far, b in (0, nt - 1)) if 0 < i < nt - 1 else (b in (0, nt - 1) and -far, far)

    targets_of = table(sent_rank)
    order = table(got_rank)
    last_of = table(lambda i, b: -b)

    def xsrc(dx):
        return lax.rem(x + dx, nx) * 2 + core

    pending = []

    def remote(src, dst, ssem, rsem, axis, index):
        return pltpu.make_async_remote_copy(
            src_ref=src, dst_ref=dst, send_sem=ssem, recv_sem=rsem,
            device_id={axis: index}, device_id_type=MESH,
        )

    def send(src, dst, ssem, rsem, axis, index):
        remote(src, dst, ssem, rsem, axis, index).start()
        pending.append((None, lambda: remote(src, dst, ssem, rsem, axis, index)))

    def arrived(dst, rsem):
        remote(dst, dst, local_sem.at[0], rsem, "src", mate).wait_recv()

    barrier = pltpu.get_barrier_semaphore()
    for j in range(1, nt):
        pl.semaphore_signal(barrier, inc=1, device_id={"tgt": order[j]}, device_id_type=MESH)
    for dx in range(1, nx):
        pl.semaphore_signal(barrier, inc=1, device_id={"src": xsrc(dx)}, device_id_type=MESH)
    pl.semaphore_signal(barrier, inc=1, device_id={"src": mate}, device_id_type=MESH)

    def cols(b):
        return pl.ds(pl.multiple_of(b * depth, 128), depth)

    def trow(lane):
        return pl.ds(pl.multiple_of(lane * rows, rows), rows)

    def drow(lane):
        return pl.ds(pl.multiple_of(lane * sub, sub), sub)

    def qrow(b):
        return pl.ds(pl.multiple_of(b * queries, queries), queries)

    def vrow(b):
        return pl.ds(pl.multiple_of(b * block, block), block)

    def erow(lane):
        return pl.ds(pl.multiple_of(lane * own, own), own)

    fetch = [
        pltpu.make_async_copy(dec_hbm, decfull.at[drow(s)], local_sem.at[1]),
        pltpu.make_async_copy(srow_hbm, srow, local_sem.at[2]),
        pltpu.make_async_copy(tpos_hbm, tpos.at[c], local_sem.at[3]),
        pltpu.make_async_copy(vproj_hbm, vproj, local_sem.at[4]),
        pltpu.make_async_copy(tgt_hbm.at[:, cols(c)], tslices.at[c, trow(s)], local_sem.at[5]),
        pltpu.make_async_copy(dec_hbm.at[:, cols(c)], dslices.at[drow(c)], local_sem.at[6]),
        pltpu.make_async_copy(oproj_hbm, oproj, local_sem.at[7]),
        pltpu.make_async_copy(attn_hbm, attn.at[:, qrow(c), :], local_sem.at[8]),
        pltpu.make_async_copy(pat_hbm, pat_ref, local_sem.at[9]),
    ]
    for cp in fetch[:7] + fetch[8:]:
        cp.start()
    pl.semaphore_wait(barrier, nt - 1 + nx)

    chunks = [(g * repeat, repeat) for g in range(groups - 1)]
    chunks += [(heads - repeat + r, 1) for r in range(repeat)]
    half = keys // 2
    lowest = half // queries if half % 128 == 0 else 0
    packed = nt - 2
    if repeat != 2 or packed < lowest or lowest == 0 or (packed + 1) * queries - half != half // 2:
        packed = -1

    def attn_copy(b, g, ssem, device, act, src=None):
        part = pl.ds(*chunks[g])

        def view(lanes):
            dst = attn.at[part, qrow(b), lanes]
            return dst if src is None else src.at[part, :, lanes], dst

        @pl.when(b < lowest)
        def _():
            a, d = view(pl.ds(0, half))
            act(remote(a, d, ssem.at[b, g], a_r.at[b, g], "tgt", device))

        if packed >= 0 and g < groups:
            @pl.when(b == packed)
            def _():
                act(remote(packs.at[g], packs.at[g], ssem.at[b, g], a_r.at[b, g], "tgt", device))

        @pl.when((b >= lowest) & (b != packed))
        def _():
            a, d = view(pl.ds(0, keys))
            act(remote(a, d, ssem.at[b, g], a_r.at[b, g], "tgt", device))

    def value_copy(b, ssem, device):
        dst = values.at[:, vrow(b), :]
        return remote(dst, dst, ssem.at[b], v_r.at[b], "tgt", device)

    start = lambda copy: copy.start()
    wait_send = lambda copy: copy.wait_send()
    wait_recv = lambda copy: copy.wait_recv()

    def rightward(act):
        pl.when(c + 1 < nt)(act)

    def leftward(act):
        pl.when(c > 0)(act)

    for dx in range(1, nx):
        send(dec_hbm, decfull.at[drow(s)], xf_s.at[dx], xf_r.at[x], "src", xsrc(dx))
    send(dec_hbm, decfull.at[drow(s)], cf_s.at[x], cf_r.at[x], "src", mate)
    def spread_copies(b):
        return (
            remote(tgt_hbm.at[:, cols(b)], tslices.at[c, trow(s)], zt_s.at[b], zt_r.at[c], "tgt", b),
            remote(tpos_hbm, tpos.at[c], zp_s.at[b], zp_r.at[c], "tgt", b),
        )

    def slice_copy(b):
        return remote(dec_hbm.at[:, cols(b)], dslices.at[drow(c)], zd_s.at[b], zd_r.at[c], "tgt", b)

    def send_slices():
        for j in range(1, nt):
            slice_copy(targets_of[j]).start()

    def spread(j):
        b = targets_of[j]
        for copy in spread_copies(b):
            copy.start()

    spread(1)
    spread(2)
    for dx in range(1, nx):
        send(tgt_hbm.at[:, cols(c)], tslices.at[c, trow(s)], xt_s.at[c, dx], xt_r.at[c, x], "src", xsrc(dx))
    send(tgt_hbm.at[:, cols(c)], tslices.at[c, trow(s)], ct_s.at[c, x], ct_r.at[c, x], "src", mate)

    fetch[1].wait()
    fetch[2].wait()
    scol_ref[...] = jnp.transpose(jnp.broadcast_to(srow[...], (128, total)))[:, :1]
    pick[...] = (scol_ref[...] == lax.broadcasted_iota(jnp.int32, (total, keys), 1)).astype(BF16)
    for b in range(lowest):
        attn[:, b * queries:(b + 1) * queries, half:] = jnp.zeros((heads, queries, keys - half), BF16)
    fetch[7].start()

    def relay(k, copy_in, copy_on):
        @pl.when(c - k >= 0)
        def _():
            copy_in(c - k)
            rightward(lambda: copy_on(c - k, 0))

        @pl.when(c + k < nt)
        def _():
            copy_in(c + k)
            leftward(lambda: copy_on(c + k, 1))

    def attn_step(k, g):
        relay(
            k, lambda b: attn_copy(b, g, ar_s, c, wait_recv),
            lambda b, left: attn_copy(b, g, al_s if left else ar_s, c - 1 if left else c + 1, start),
        )

    def value_step(k):
        relay(
            k, lambda b: value_copy(b, vr_s, c).wait_recv(),
            lambda b, left: value_copy(b, vl_s if left else vr_s, c - 1 if left else c + 1).start(),
        )

    def take(j):
        b = order[j]
        arrived(tslices.at[b, trow(s)], zt_r.at[b])
        for dx in range(1, nx):
            send(tslices.at[b, trow(s)], tslices.at[b, trow(s)], xt_s.at[b, dx], xt_r.at[b, x], "src", xsrc(dx))
        send(tslices.at[b, trow(s)], tslices.at[b, trow(s)], ct_s.at[b, x], ct_r.at[b, x], "src", mate)

    fetch[0].wait()
    for dx in range(1, nx):
        z = lax.rem(x + dx, nx)
        y = xsrc(dx)
        arrived(decfull.at[drow(y)], xf_r.at[z])
        send(decfull.at[drow(y)], decfull.at[drow(y)], cf_s.at[z], cf_r.at[z], "src", mate)
    for dx in range(nx):
        z = lax.rem(x + dx, nx)
        arrived(decfull.at[drow(z * 2 + 1 - core)], cf_r.at[z])
    fetch[3].wait()

    @pl.loop(0, groups)
    def _(g):
        values[g, vrow(c)] = dot(decfull[...], vproj[g]).astype(BF16)

    fetch[7].wait()
    if packed >= 0:
        @pl.when(c == packed)
        def _():
            at = slice(packed * queries, (packed + 1) * queries)
            for g in range(groups):
                packs[g, 0] = attn[2 * g, at, :half]
                packs[g, 1] = attn[2 * g + 1, at, :half]
                packs[g, 2] = jnp.concatenate(
                    [attn[2 * g + r, at, half:half + half // 2] for r in range(2)], axis=1
                )
    rightward(lambda: value_copy(c, vr_s, c + 1).start())
    leftward(lambda: value_copy(c, vl_s, c - 1).start())

    def cross(j):
        b = order[j]
        for dx in range(1, nx):
            z = lax.rem(x + dx, nx)
            y = z * 2 + core
            arrived(tslices.at[b, trow(y)], xt_r.at[b, z])
            send(tslices.at[b, trow(y)], tslices.at[b, trow(y)], ct_s.at[b, z], ct_r.at[b, z], "src", mate)

    def ready(j):
        b = order[j]
        if j == 0:
            fetch[4].wait()
            fetch[6].wait()
        else:
            arrived(tpos.at[b], zp_r.at[b])
        for dx in range(nx):
            z = lax.rem(x + dx, nx)
            arrived(tslices.at[b, trow(z * 2 + 1 - core)], ct_r.at[b, z])

    def read_block(j, part):
        b = order[j]
        share = groups // 2

        @pl.loop(part * share, groups if part else share)
        def _(g):
            pair = jnp.concatenate([oproj[g * repeat + r] for r in range(repeat)], axis=1)
            reads[b, g] = dot(tslices[b], pair).astype(BF16)

        if part:
            onehot[b] = (
                lax.broadcasted_iota(jnp.int32, (nt * queries, targets), 0) == tpos[b]
            ).astype(BF16)

    def wait_slices():
        fetch[5].wait()
        for j in range(1, nt):
            arrived(dslices.at[drow(order[j])], zd_r.at[order[j]])

    def add_direct(b):
        direct = dot_nt(dslices[...], tslices[b])
        here = tpos[b]
        for p in range(nt):
            at = pl.ds(pl.multiple_of(p * block + s * sub, sub), sub)
            same = (scol_ref[at] == here).astype(F32)
            edges[b, at] += direct[p * sub:(p + 1) * sub] * same

    def unpack(g):
        at = slice(packed * queries, (packed + 1) * queries)
        both = packs[g, 2].astype(F32)
        lane = lax.broadcasted_iota(jnp.int32, both.shape, 1)
        for r in range(2):
            attn[2 * g + r, at, :half] = packs[g, r]
            upper = pltpu.roll(both, half // 2, 1) if r else both
            attn[2 * g + r, at, half:] = jnp.where(lane < half // 2, upper, 0.0).astype(BF16)

    def pick_keys(i):
        if packed >= 0 and i < groups:
            pl.when(c != packed)(lambda: unpack(i))
        for h in range(chunks[i][0], sum(chunks[i])):
            attn_n[h] = dot_nt(pick[...], attn[h]).astype(BF16)

    def issue(g):
        rightward(lambda: attn_copy(c, g, ar_s, c + 1, start, attn_hbm))
        leftward(lambda: attn_copy(c, g, al_s, c - 1, start, attn_hbm))

    def mix_all(g):
        for j in range(nt):
            mix(g, last_of[j])

    def add_all():
        for j in range(nt):
            add_direct(last_of[j])

    def mix(i, b):
        terms = None
        for h in range(chunks[i][0], sum(chunks[i])):
            g, r = h // repeat, h % repeat
            term = dot(attn_n[h], onehot[b]) * dot_nt(values[g], reads[b, g, :, r * hd:(r + 1) * hd])
            terms = term if terms is None else terms + term
        edges[b] = terms if i == 0 else edges[b] + terms

    def to_mate(b):
        for z in range(nx):
            send(edges.at[b, erow(z * 2 + 1 - core)], core_in.at[b, z], ce_s.at[b, z], ce_r.at[b, z], "src", mate)

    def over_x(b):
        for dx in range(1, nx):
            z = lax.rem(x + dx, nx)
            arrived(core_in.at[b, z], ce_r.at[b, z])
            x_out[b, z] = (edges[b, erow(z * 2 + core)] + core_in[b, z]).astype(BF16)
            send(x_out.at[b, z], x_in.at[b, x], xe_s.at[b, z], xe_r.at[b, x], "src", z * 2 + core)
        arrived(core_in.at[b, x], ce_r.at[b, x])

    def over_z(b, away):
        mine = edges[b, erow(s)] + core_in[b, x]
        for dx in range(1, nx):
            z = lax.rem(x + dx, nx)
            arrived(x_in.at[b, z], xe_r.at[b, z])
            mine += x_in[b, z].astype(F32)
        if away:
            z_out[b] = mine.astype(BF16)
            send(z_out.at[b], z_in.at[c], ze_s.at[b], ze_r.at[c], "tgt", b)
        return mine

    spread(3)
    issue(0)
    take(1)
    issue(1)
    take(2)
    cross(0)
    issue(2)
    cross(1)
    value_step(1)
    ready(0)
    take(3)
    issue(3)
    read_block(0, 1)
    ready(1)
    read_block(1, 0)
    attn_step(1, 0)
    issue(4)
    read_block(0, 0)
    attn_step(1, 1)
    read_block(1, 1)
    attn_step(1, 2)
    value_step(2)
    attn_step(1, 3)
    cross(2)
    ready(2)
    attn_step(2, 0)
    read_block(2, 1)
    send_slices()
    cross(3)
    value_step(3)
    attn_step(2, 1)
    read_block(2, 0)
    ready(3)
    read_block(3, 1)
    attn_step(3, 0)
    pick_keys(0)
    read_block(3, 0)
    attn_step(1, 4)
    mix_all(0)
    attn_step(2, 2)
    attn_step(3, 1)
    pick_keys(1)
    attn_step(2, 3)
    mix_all(1)
    wait_slices()
    add_all()
    attn_step(3, 2)
    pick_keys(2)
    mix_all(2)
    attn_step(2, 4)
    attn_step(3, 3)
    pick_keys(3)
    mix_all(3)
    attn_step(3, 4)
    last = len(chunks) - 1
    pick_keys(last)
    mix(last, last_of[1])
    to_mate(last_of[1])
    mix(last, last_of[2])
    to_mate(last_of[2])
    for j in range(3, nt):
        mix(last, last_of[j])
        to_mate(last_of[j])
        over_x(last_of[j - 2])
    mix(last, c)
    to_mate(c)
    over_x(last_of[nt - 2])
    over_x(last_of[nt - 1])
    over_x(c)
    for j in range(1, nt):
        over_z(last_of[j], True)
    mine = over_z(c, False)
    fetch[8].wait()
    for j in range(1, nt):
        for copy in spread_copies(order[j]) + (slice_copy(order[j]),):
            copy.wait_send()
    for _, again in pending:
        again().wait_send()
    for k in range(nt):
        @pl.when((c - k >= 0) & (c + 1 < nt))
        def _():
            for g in range(len(chunks)):
                attn_copy(c - k, g, ar_s, c + 1, wait_send)
            value_copy(c - k, vr_s, c + 1).wait_send()

        @pl.when((c + k < nt) & (c > 0))
        def _():
            for g in range(len(chunks)):
                attn_copy(c + k, g, al_s, c - 1, wait_send)
            value_copy(c + k, vl_s, c - 1).wait_send()

    for j in range(1, nt):
        b = order[j]
        arrived(z_in.at[b], ze_r.at[b])
        mine += z_in[b].astype(F32)
    kept = pat_ref[(s * own) // block, c]
    out_ref[...] = (mine * kept.astype(F32)).astype(BF16)


def resident_shards(
    target_rows, target_pos, decoder_rows, source_pos, out_proj, value_proj, attention, tile_pattern
):
    nt, ns = lax.axis_size("tgt"), lax.axis_size("src")
    rows = target_rows.shape[0]
    sub, width = decoder_rows.shape
    heads, depth, head_dim = out_proj.shape
    groups = value_proj.shape[0]
    repeat = heads // groups
    _, queries, keys = attention.shape
    total = source_pos.shape[0]
    targets = target_pos.shape[0]
    own = total // ns
    nx = ns // 2
    vmem = pl.BlockSpec(memory_space=pltpu.VMEM)
    hbm = pl.BlockSpec(memory_space=pl.ANY)
    sem = lambda *shape: pltpu.SemaphoreType.DMA(shape)
    return pl.pallas_call(
        functools.partial(edge_kernel, nt, ns),
        out_shape=pltpu.VMEM((own, targets), BF16),
        in_specs=[hbm] * 8,
        out_specs=vmem,
        scratch_shapes=[
            pltpu.VMEM(out_proj.shape, BF16),
            pltpu.VMEM(value_proj.shape, BF16),
            pltpu.VMEM((nt, ns * rows, depth), BF16),
            pltpu.VMEM((nt * sub, depth), BF16),
            pltpu.VMEM((ns * sub, width), BF16),
            pltpu.VMEM((heads, nt * queries, keys), BF16),
            pltpu.VMEM((groups, 3, queries, keys // 2), BF16),
            pltpu.VMEM((nt, 1, targets), jnp.int32),
            pltpu.VMEM((1, total), jnp.int32),
            pltpu.VMEM((groups, total, head_dim), BF16),
            pltpu.VMEM((nt, groups, targets, repeat * head_dim), BF16),
            pltpu.VMEM((total, keys), BF16),
            pltpu.VMEM((heads, total, nt * queries), BF16),
            pltpu.VMEM((nt, nt * queries, targets), BF16),
            pltpu.VMEM((nt, total, targets), F32),
            pltpu.VMEM((nt, nx, own, targets), F32),
            pltpu.VMEM((nt, nx, own, targets), BF16),
            pltpu.VMEM((nt, nx, own, targets), BF16),
            pltpu.VMEM((nt, own, targets), BF16),
            pltpu.VMEM((nt, own, targets), BF16),
            pltpu.VMEM((total, 1), jnp.int32),
            pltpu.SMEM(tile_pattern.shape, jnp.int32),
            sem(10),
            sem(nt), sem(nt), sem(nt), sem(nt), sem(nt), sem(nt),
            sem(nt, groups + repeat - 1), sem(nt, groups + repeat - 1), sem(nt, groups + repeat - 1), sem(nt), sem(nt), sem(nt),
            sem(nt, nx), sem(nt, nx), sem(nt, nx), sem(nt, nx),
            sem(nx), sem(nx), sem(nx), sem(nx),
            sem(nt, nx), sem(nt, nx), sem(nt, nx), sem(nt, nx), sem(nt), sem(nt),
        ],
        compiler_params=pltpu.CompilerParams(
            collective_id=0, has_side_effects=True, vmem_limit_bytes=60 * 1024 * 1024
        ),
    )(
        target_rows, target_pos.reshape(1, targets), decoder_rows, source_pos.reshape(1, total),
        out_proj, value_proj, attention, tile_pattern,
    )


def resident_bytes(nt, ns, width, heads, depth, groups, rows, total, targets):
    weights = heads * depth * 128 + groups * width * 128
    gathered = nt * ns * rows * depth + nt * heads * targets * 128
    return 2 * (weights + gathered) + 4 * nt * total * targets * 2


def shards(
    target_rows, target_pos, decoder_rows, source_pos, out_proj, value_proj, attention, tile_pattern
):
    nt, ns = lax.axis_size("tgt"), lax.axis_size("src")
    heads, depth, head_dim = out_proj.shape
    need = resident_bytes(
        nt, ns, target_rows.shape[1], heads, depth, value_proj.shape[0], target_rows.shape[0],
        source_pos.shape[0], target_pos.shape[0],
    )
    fits = (
        depth % 128 == 0 and head_dim == 128 and ns % 2 == 0 and nt > 2
        and decoder_rows.shape[0] % 16 == 0 and attention.shape[1] % 16 == 0
        and need < 40 * 1024 * 1024
    )
    plan = resident_shards if fits else gathered_shards
    return plan(
        target_rows, target_pos, decoder_rows, source_pos, out_proj, value_proj, attention, tile_pattern
    )


def solution(mesh):
    return jax.shard_map(
        shards,
        mesh=mesh,
        in_specs=(
            P(("grp", "tgt", "src"), None),
            P(("grp", "tgt")),
            P(("grp", "tgt", "src"), None),
            P("grp"),
            P("src", "tgt", None),
            P("src", None, None),
            P(("grp", "src"), "tgt", None),
            P("grp", None),
        ),
        out_specs=P(("grp", "src"), "tgt"),
        check_vma=False,
    )
```

```python
import functools

import jax
import jax.numpy as jnp
from jax import lax
from jax.experimental import pallas as pl
from jax.experimental.pallas import tpu as pltpu
from jax.sharding import PartitionSpec as P


def passed_along(value, axis, steps):
    count = lax.axis_size(axis)
    pairs = [(source, (source + steps) % count) for source in range(count)]
    return lax.ppermute(value, axis, pairs)


def gathered_shards(
    target_rows, target_pos, decoder_rows, source_pos, out_proj, value_proj, attention, tile_pattern
):
    blocks = lax.axis_size("tgt")
    column = lax.axis_index("tgt")
    src_lane = lax.axis_index("src")
    full_targets, full_sources = (
        lax.all_gather(target_rows, "src", axis=0, tiled=True),
        lax.all_gather(decoder_rows, "src", axis=0, tiled=True),
    )
    tgt_dev = full_targets.shape[0]
    src_dev = full_sources.shape[0]
    sub_rows = decoder_rows.shape[0]
    heads_here = out_proj.shape[0]
    head_dim = out_proj.shape[2]
    groups_here = value_proj.shape[0]
    repeat = heads_here // groups_here
    read_sum = jnp.einsum(
        "td,hde->the",
        full_targets,
        lax.all_gather(out_proj, "tgt", axis=1, tiled=True),
        preferred_element_type=jnp.float32,
    )
    head_reads = read_sum.astype(jnp.bfloat16).reshape(tgt_dev, groups_here, repeat, head_dim)
    values = jnp.einsum("sd,gde->sge", full_sources, value_proj, preferred_element_type=jnp.float32)
    values = values.astype(jnp.bfloat16).reshape(src_dev, groups_here * head_dim)
    attn_table = lax.all_gather(attention, "tgt", axis=1, tiled=True)
    target_attn = jnp.take(attn_table, target_pos, axis=1)
    keyed_attn = jnp.transpose(target_attn, (0, 2, 1))

    def edge_tile(payload, block_index):
        decoder_part, value_part = payload
        key_positions = lax.dynamic_slice_in_dim(source_pos, block_index * src_dev, src_dev)
        weights = jnp.take(keyed_attn, key_positions, axis=1).astype(jnp.float32)
        scores = jnp.einsum(
            "sgd,tgrd->grst",
            value_part.reshape(src_dev, groups_here, head_dim),
            head_reads,
            preferred_element_type=jnp.float32,
        )
        scores = scores.reshape(heads_here, src_dev, tgt_dev)
        mixed_term = jnp.sum(weights * scores, axis=0)
        own_positions = lax.dynamic_slice_in_dim(key_positions, src_lane * sub_rows, sub_rows)
        same_place = (own_positions[:, None] == target_pos[None, :]).astype(jnp.float32)
        direct = (
            jnp.einsum("sd,td->st", decoder_part, full_targets, preferred_element_type=jnp.float32)
            * same_place
        )
        own_rows = lax.dynamic_slice_in_dim(mixed_term, src_lane * sub_rows, sub_rows, 0)
        return lax.dynamic_update_slice_in_dim(
            mixed_term, own_rows + direct, src_lane * sub_rows, 0
        )

    def place_tile(partial_value, payload, block_index):
        kept_flag = tile_pattern[block_index, column]
        piece_tile = edge_tile(payload, block_index) * kept_flag.astype(jnp.float32)
        return lax.dynamic_update_slice_in_dim(partial_value, piece_tile, block_index * src_dev, 0)

    own_block = (decoder_rows, values)
    partial_value = jnp.zeros((blocks * src_dev, tgt_dev), jnp.float32)
    partial_value = place_tile(partial_value, own_block, column)

    def cycle_turn(turn_index, state_carry):
        forward_block, backward_block, running = state_carry
        forward_block = passed_along((forward_block[0], forward_block[1]), "tgt", 1)
        backward_block = passed_along((backward_block[0], backward_block[1]), "tgt", -1)
        running = place_tile(running, forward_block, (column - turn_index) % blocks)
        running = place_tile(running, backward_block, (column + turn_index) % blocks)
        return (forward_block, backward_block, running)

    forward_block, backward_block, partial_value = lax.fori_loop(
        1, blocks // 2, cycle_turn, (own_block, own_block, partial_value)
    )
    forward_block = passed_along((forward_block[0], forward_block[1]), "tgt", 1)
    partial_value = place_tile(partial_value, forward_block, (column - blocks // 2) % blocks)
    summed = lax.psum_scatter(partial_value, "src", scatter_dimension=0, tiled=True)
    return summed.astype(jnp.bfloat16)


F32 = jnp.float32
BF16 = jnp.bfloat16
MESH = pl.DeviceIdType.MESH


def dot(a, b):
    return jnp.dot(a, b, preferred_element_type=F32)


def dot_nt(a, b):
    return lax.dot_general(a, b, (((1,), (1,)), ((), ())), preferred_element_type=F32)


def edge_kernel(
    nt, ns, tgt_hbm, tpos_hbm, dec_hbm, srow_hbm, oproj_hbm, vproj_hbm, attn_hbm, pat_hbm,
    out_ref,
    oproj, vproj, tslices, dslices, decfull, attn, packs, tpos, srow, values, reads, pick, attn_n, onehot,
    edges, core_in, x_out, x_in, z_out, z_in, scol_ref, pat_ref,
    local_sem, zt_s, zt_r, zd_s, zd_r, zp_s, zp_r, ar_s, al_s, a_r, vr_s, vl_s, v_r,
    xt_s, xt_r, ct_s, ct_r, xf_s, xf_r, cf_s, cf_r, ce_s, ce_r, xe_s, xe_r, ze_s, ze_r,
):
    c = lax.axis_index("tgt")
    s = lax.axis_index("src")
    nx = ns // 2
    x = s // 2
    core = s % 2
    mate = x * 2 + 1 - core
    rows, depth = tslices.shape[1] // ns, tslices.shape[2]
    sub = dec_hbm.shape[0]
    heads = oproj.shape[0]
    groups = vproj.shape[0]
    repeat = heads // groups
    block = sub * ns
    queries, keys = attn_hbm.shape[1:]
    targets = tpos.shape[2]
    total = scol_ref.shape[0]
    own = edges.shape[1] // ns
    hd = vproj.shape[2]

    inner = (c > 0) & (c + 1 < nt)

    def table(rank):
        rows_of = [[i] + sorted((b for b in range(nt) if b != i), key=lambda b: rank(i, b)) for i in range(nt)]

        def entry(j):
            b = rows_of[0][j]
            for i in range(1, nt):
                b = jnp.where(c == i, rows_of[i][j], b)
            return b

        return [entry(j) for j in range(nt)]

    def sent_rank(i, b):
        return abs(b - i) if 0 < i < nt - 1 else -abs(b - i)

    def got_rank(i, b):
        far = abs(b - i)
        return (-far, b in (0, nt - 1)) if 0 < i < nt - 1 else (b in (0, nt - 1) and -far, far)

    targets_of = table(sent_rank)
    order = table(got_rank)
    last_of = table(lambda i, b: -b)

    def xsrc(dx):
        return lax.rem(x + dx, nx) * 2 + core

    def remote(src, dst, ssem, rsem, axis, index):
        return pltpu.make_async_remote_copy(
            src_ref=src, dst_ref=dst, send_sem=ssem, recv_sem=rsem,
            device_id={axis: index}, device_id_type=MESH,
        )

    def send(src, dst, ssem, rsem, axis, index):
        remote(src, dst, ssem, rsem, axis, index).start()

    def arrived(dst, rsem):
        remote(dst, dst, local_sem.at[0], rsem, "src", mate).wait_recv()

    barrier = pltpu.get_barrier_semaphore()
    for j in range(1, nt):
        pl.semaphore_signal(barrier, inc=1, device_id={"tgt": order[j]}, device_id_type=MESH)
    for dx in range(1, nx):
        pl.semaphore_signal(barrier, inc=1, device_id={"src": xsrc(dx)}, device_id_type=MESH)
    pl.semaphore_signal(barrier, inc=1, device_id={"src": mate}, device_id_type=MESH)

    def cols(b):
        return pl.ds(pl.multiple_of(b * depth, 128), depth)

    def trow(lane):
        return pl.ds(pl.multiple_of(lane * rows, rows), rows)

    def drow(lane):
        return pl.ds(pl.multiple_of(lane * sub, sub), sub)

    def qrow(b):
        return pl.ds(pl.multiple_of(b * queries, queries), queries)

    def vrow(b):
        return pl.ds(pl.multiple_of(b * block, block), block)

    def erow(lane):
        return pl.ds(pl.multiple_of(lane * own, own), own)

    fetch = [
        pltpu.make_async_copy(dec_hbm, decfull.at[drow(s)], local_sem.at[1]),
        pltpu.make_async_copy(srow_hbm, srow, local_sem.at[2]),
        pltpu.make_async_copy(tpos_hbm, tpos.at[c], local_sem.at[3]),
        pltpu.make_async_copy(vproj_hbm, vproj, local_sem.at[4]),
        pltpu.make_async_copy(tgt_hbm.at[:, cols(c)], tslices.at[c, trow(s)], local_sem.at[5]),
        pltpu.make_async_copy(dec_hbm.at[:, cols(c)], dslices.at[drow(c)], local_sem.at[6]),
        pltpu.make_async_copy(oproj_hbm, oproj, local_sem.at[7]),
        pltpu.make_async_copy(attn_hbm, attn.at[:, qrow(c), :], local_sem.at[8]),
        pltpu.make_async_copy(pat_hbm, pat_ref, local_sem.at[9]),
    ]
    for cp in fetch[:7] + fetch[8:]:
        cp.start()
    pl.semaphore_wait(barrier, nt - 1 + nx)

    chunks = [(g * repeat, repeat) for g in range(groups - 1)]
    chunks += [(heads - repeat + r, 1) for r in range(repeat)]
    half = keys // 2
    lowest = half // queries if half % 128 == 0 else 0
    packed = nt - 2
    if repeat != 2 or packed < lowest or lowest == 0 or (packed + 1) * queries - half != half // 2:
        packed = -1

    def attn_copy(b, g, ssem, device, act, src=None):
        part = pl.ds(*chunks[g])

        def view(lanes):
            dst = attn.at[part, qrow(b), lanes]
            return dst if src is None else src.at[part, :, lanes], dst

        @pl.when(b < lowest)
        def _():
            a, d = view(pl.ds(0, half))
            act(remote(a, d, ssem.at[0], a_r.at[b, g], "tgt", device))

        if packed >= 0 and g < groups:
            @pl.when(b == packed)
            def _():
                act(remote(packs.at[g], packs.at[g], ssem.at[0], a_r.at[b, g], "tgt", device))

        @pl.when((b >= lowest) & (b != packed))
        def _():
            a, d = view(pl.ds(0, keys))
            act(remote(a, d, ssem.at[0], a_r.at[b, g], "tgt", device))

    def value_copy(b, ssem, device):
        dst = values.at[:, vrow(b), :]
        return remote(dst, dst, ssem.at[0], v_r.at[b], "tgt", device)

    start = lambda copy: copy.start()
    wait_send = lambda copy: copy.wait_send()
    wait_recv = lambda copy: copy.wait_recv()

    def rightward(act):
        pl.when(c + 1 < nt)(act)

    def leftward(act):
        pl.when(c > 0)(act)

    for dx in range(1, nx):
        send(dec_hbm, decfull.at[drow(s)], xf_s.at[0], xf_r.at[x], "src", xsrc(dx))
    send(dec_hbm, decfull.at[drow(s)], cf_s.at[0], cf_r.at[x], "src", mate)
    def spread_copies(b):
        return (
            remote(tgt_hbm.at[:, cols(b)], tslices.at[c, trow(s)], zt_s.at[0], zt_r.at[c], "tgt", b),
            remote(tpos_hbm, tpos.at[c], zp_s.at[0], zp_r.at[c], "tgt", b),
        )

    def slice_copy(b):
        return remote(dec_hbm.at[:, cols(b)], dslices.at[drow(c)], zd_s.at[0], zd_r.at[0], "tgt", b)

    def send_slices():
        for j in range(1, nt):
            slice_copy(targets_of[j]).start()

    def spread(j):
        b = targets_of[j]
        for copy in spread_copies(b):
            copy.start()

    spread(1)
    spread(2)
    for dx in range(1, nx):
        send(tgt_hbm.at[:, cols(c)], tslices.at[c, trow(s)], xt_s.at[0], xt_r.at[c, x], "src", xsrc(dx))
    send(tgt_hbm.at[:, cols(c)], tslices.at[c, trow(s)], ct_s.at[0], ct_r.at[c, x], "src", mate)

    fetch[1].wait()
    fetch[2].wait()
    scol_ref[...] = jnp.transpose(jnp.broadcast_to(srow[...], (128, total)))[:, :1]
    pick[...] = (scol_ref[...] == lax.broadcasted_iota(jnp.int32, (total, keys), 1)).astype(BF16)
    for b in range(lowest):
        attn[:, b * queries:(b + 1) * queries, half:] = jnp.zeros((heads, queries, keys - half), BF16)
    fetch[7].start()

    def relay(k, copy_in, copy_on):
        @pl.when(c - k >= 0)
        def _():
            copy_in(c - k)
            rightward(lambda: copy_on(c - k, 0))

        @pl.when(c + k < nt)
        def _():
            copy_in(c + k)
            leftward(lambda: copy_on(c + k, 1))

    def attn_step(k, g):
        relay(
            k, lambda b: attn_copy(b, g, ar_s, c, wait_recv),
            lambda b, left: attn_copy(b, g, al_s if left else ar_s, c - 1 if left else c + 1, start),
        )

    def value_step(k):
        relay(
            k, lambda b: value_copy(b, vr_s, c).wait_recv(),
            lambda b, left: value_copy(b, vl_s if left else vr_s, c - 1 if left else c + 1).start(),
        )

    def take(j):
        b = order[j]
        arrived(tslices.at[b, trow(s)], zt_r.at[b])
        for dx in range(1, nx):
            send(tslices.at[b, trow(s)], tslices.at[b, trow(s)], xt_s.at[0], xt_r.at[b, x], "src", xsrc(dx))
        send(tslices.at[b, trow(s)], tslices.at[b, trow(s)], ct_s.at[0], ct_r.at[b, x], "src", mate)

    fetch[0].wait()
    for dx in range(1, nx):
        z = lax.rem(x + dx, nx)
        y = xsrc(dx)
        arrived(decfull.at[drow(y)], xf_r.at[z])
        send(decfull.at[drow(y)], decfull.at[drow(y)], cf_s.at[0], cf_r.at[z], "src", mate)
    for dx in range(nx):
        z = lax.rem(x + dx, nx)
        arrived(decfull.at[drow(z * 2 + 1 - core)], cf_r.at[z])
    fetch[3].wait()

    @pl.loop(0, groups)
    def _(g):
        values[g, vrow(c)] = dot(decfull[...], vproj[g]).astype(BF16)

    fetch[7].wait()
    if packed >= 0:
        @pl.when(c == packed)
        def _():
            at = slice(packed * queries, (packed + 1) * queries)
            for g in range(groups):
                packs[g, 0] = attn[2 * g, at, :half]
                packs[g, 1] = attn[2 * g + 1, at, :half]
                packs[g, 2] = jnp.concatenate(
                    [attn[2 * g + r, at, half:half + half // 2] for r in range(2)], axis=1
                )
    rightward(lambda: value_copy(c, vr_s, c + 1).start())
    leftward(lambda: value_copy(c, vl_s, c - 1).start())

    def cross(j):
        b = order[j]
        for dx in range(1, nx):
            z = lax.rem(x + dx, nx)
            y = z * 2 + core
            arrived(tslices.at[b, trow(y)], xt_r.at[b, z])
            send(tslices.at[b, trow(y)], tslices.at[b, trow(y)], ct_s.at[0], ct_r.at[b, z], "src", mate)

    def ready(j):
        b = order[j]
        if j == 0:
            fetch[4].wait()
            fetch[6].wait()
        else:
            arrived(tpos.at[b], zp_r.at[b])
        for dx in range(nx):
            z = lax.rem(x + dx, nx)
            arrived(tslices.at[b, trow(z * 2 + 1 - core)], ct_r.at[b, z])

    def read_block(j, part):
        b = order[j]
        share = groups // 2

        @pl.loop(part * share, groups if part else share)
        def _(g):
            pair = jnp.concatenate([oproj[g * repeat + r] for r in range(repeat)], axis=1)
            reads[b, g] = dot(tslices[b], pair).astype(BF16)

        if part:
            onehot[b] = (
                lax.broadcasted_iota(jnp.int32, (nt * queries, targets), 0) == tpos[b]
            ).astype(BF16)

    def wait_slices():
        fetch[5].wait()
        arrived(dslices.at[:(nt - 1) * sub], zd_r.at[0])

    def add_direct(b):
        direct = dot_nt(dslices[...], tslices[b])
        here = tpos[b]
        for p in range(nt):
            at = pl.ds(pl.multiple_of(p * block + s * sub, sub), sub)
            same = (scol_ref[at] == here).astype(F32)
            edges[b, at] += direct[p * sub:(p + 1) * sub] * same

    def unpack(g):
        at = slice(packed * queries, (packed + 1) * queries)
        both = packs[g, 2].astype(F32)
        lane = lax.broadcasted_iota(jnp.int32, both.shape, 1)
        for r in range(2):
            attn[2 * g + r, at, :half] = packs[g, r]
            upper = pltpu.roll(both, half // 2, 1) if r else both
            attn[2 * g + r, at, half:] = jnp.where(lane < half // 2, upper, 0.0).astype(BF16)

    def pick_keys(i):
        if packed >= 0 and i < groups:
            pl.when(c != packed)(lambda: unpack(i))
        for h in range(chunks[i][0], sum(chunks[i])):
            attn_n[h] = dot_nt(pick[...], attn[h]).astype(BF16)

    def issue(g):
        rightward(lambda: attn_copy(c, g, ar_s, c + 1, start, attn_hbm))
        leftward(lambda: attn_copy(c, g, al_s, c - 1, start, attn_hbm))

    def mix_all(g):
        for j in range(nt):
            mix(g, last_of[j])

    def add_all():
        for j in range(nt):
            add_direct(last_of[j])

    def mix(i, b):
        terms = None
        for h in range(chunks[i][0], sum(chunks[i])):
            g, r = h // repeat, h % repeat
            term = dot(attn_n[h], onehot[b]) * dot_nt(values[g], reads[b, g, :, r * hd:(r + 1) * hd])
            terms = term if terms is None else terms + term
        edges[b] = terms if i == 0 else edges[b] + terms

    def to_mate(b):
        for z in range(nx):
            send(edges.at[b, erow(z * 2 + 1 - core)], core_in.at[b, z], ce_s.at[0], ce_r.at[b, z], "src", mate)

    def over_x(b):
        for dx in range(1, nx):
            z = lax.rem(x + dx, nx)
            arrived(core_in.at[b, z], ce_r.at[b, z])
            x_out[b, z] = (edges[b, erow(z * 2 + core)] + core_in[b, z]).astype(BF16)
            send(x_out.at[b, z], x_in.at[b, x], xe_s.at[0], xe_r.at[b, x], "src", z * 2 + core)
        arrived(core_in.at[b, x], ce_r.at[b, x])

    def over_z(b, away):
        mine = edges[b, erow(s)] + core_in[b, x]
        for dx in range(1, nx):
            z = lax.rem(x + dx, nx)
            arrived(x_in.at[b, z], xe_r.at[b, z])
            mine += x_in[b, z].astype(F32)
        if away:
            z_out[b] = mine.astype(BF16)
            send(z_out.at[b], z_in.at[c], ze_s.at[0], ze_r.at[0], "tgt", b)
        return mine

    spread(3)
    issue(0)
    take(1)
    issue(1)
    take(2)
    cross(0)
    issue(2)
    cross(1)
    value_step(1)
    ready(0)
    take(3)
    issue(3)
    read_block(0, 1)
    ready(1)
    read_block(1, 0)
    attn_step(1, 0)
    issue(4)
    read_block(0, 0)
    attn_step(1, 1)
    read_block(1, 1)
    attn_step(1, 2)
    value_step(2)
    attn_step(1, 3)
    cross(2)
    ready(2)
    attn_step(2, 0)
    read_block(2, 1)
    send_slices()
    cross(3)
    value_step(3)
    attn_step(2, 1)
    read_block(2, 0)
    ready(3)
    read_block(3, 1)
    attn_step(3, 0)
    pick_keys(0)
    read_block(3, 0)
    attn_step(1, 4)
    mix_all(0)
    attn_step(2, 2)
    attn_step(3, 1)
    pick_keys(1)
    attn_step(2, 3)
    mix_all(1)
    wait_slices()
    add_all()
    attn_step(3, 2)
    pick_keys(2)
    mix_all(2)
    attn_step(2, 4)
    attn_step(3, 3)
    pick_keys(3)
    mix_all(3)
    attn_step(3, 4)
    last = len(chunks) - 1
    pick_keys(last)
    mix(last, last_of[1])
    to_mate(last_of[1])
    mix(last, last_of[2])
    to_mate(last_of[2])
    for j in range(3, nt):
        mix(last, last_of[j])
        to_mate(last_of[j])
        over_x(last_of[j - 2])
    mix(last, c)
    to_mate(c)
    over_x(last_of[nt - 2])
    over_x(last_of[nt - 1])
    over_x(c)
    for j in range(1, nt):
        over_z(last_of[j], True)
    mine = over_z(c, False)
    fetch[8].wait()
    def drained(view, ssem):
        remote(view, view, ssem.at[0], local_sem.at[0], "src", mate).wait_send()

    drained(tslices.at[:nt - 1, :rows], zt_s)
    drained(tslices.at[:, :(nx - 1) * rows], xt_s)
    drained(tslices.at[:, :nx * rows], ct_s)
    drained(dslices.at[:(nt - 1) * sub], zd_s)
    drained(tpos.at[:nt - 1], zp_s)
    drained(decfull.at[:(nx - 1) * sub], xf_s)
    drained(decfull.at[:nx * sub], cf_s)
    drained(core_in, ce_s)
    drained(x_out.at[:, :nx - 1], xe_s)
    drained(z_out.at[:nt - 1], ze_s)

    def tiles(b):
        return heads if b < lowest else 3 * groups if b == packed else 2 * heads

    for i in range(nt):
        @pl.when(c == i)
        def _():
            if i + 1 < nt:
                drained(vproj.at[0, :queries * sum(tiles(b) for b in range(i + 1))], ar_s)
                drained(values.at[:, :(i + 1) * block], vr_s)
            if i > 0:
                drained(vproj.at[0, :queries * sum(tiles(b) for b in range(i, nt))], al_s)
                drained(values.at[:, :(nt - i) * block], vl_s)

    arrived(z_in.at[:nt - 1], ze_r.at[0])
    for j in range(1, nt):
        mine += z_in[order[j]].astype(F32)
    kept = pat_ref[(s * own) // block, c]
    out_ref[...] = (mine * kept.astype(F32)).astype(BF16)


def resident_shards(
    target_rows, target_pos, decoder_rows, source_pos, out_proj, value_proj, attention, tile_pattern
):
    nt, ns = lax.axis_size("tgt"), lax.axis_size("src")
    rows = target_rows.shape[0]
    sub, width = decoder_rows.shape
    heads, depth, head_dim = out_proj.shape
    groups = value_proj.shape[0]
    repeat = heads // groups
    _, queries, keys = attention.shape
    total = source_pos.shape[0]
    targets = target_pos.shape[0]
    own = total // ns
    nx = ns // 2
    vmem = pl.BlockSpec(memory_space=pltpu.VMEM)
    hbm = pl.BlockSpec(memory_space=pl.ANY)
    sem = lambda *shape: pltpu.SemaphoreType.DMA(shape)
    return pl.pallas_call(
        functools.partial(edge_kernel, nt, ns),
        out_shape=pltpu.VMEM((own, targets), BF16),
        in_specs=[hbm] * 8,
        out_specs=vmem,
        scratch_shapes=[
            pltpu.VMEM(out_proj.shape, BF16),
            pltpu.VMEM(value_proj.shape, BF16),
            pltpu.VMEM((nt, ns * rows, depth), BF16),
            pltpu.VMEM((nt * sub, depth), BF16),
            pltpu.VMEM((ns * sub, width), BF16),
            pltpu.VMEM((heads, nt * queries, keys), BF16),
            pltpu.VMEM((groups, 3, queries, keys // 2), BF16),
            pltpu.VMEM((nt, 1, targets), jnp.int32),
            pltpu.VMEM((1, total), jnp.int32),
            pltpu.VMEM((groups, total, head_dim), BF16),
            pltpu.VMEM((nt, groups, targets, repeat * head_dim), BF16),
            pltpu.VMEM((total, keys), BF16),
            pltpu.VMEM((heads, total, nt * queries), BF16),
            pltpu.VMEM((nt, nt * queries, targets), BF16),
            pltpu.VMEM((nt, total, targets), F32),
            pltpu.VMEM((nt, nx, own, targets), F32),
            pltpu.VMEM((nt, nx, own, targets), BF16),
            pltpu.VMEM((nt, nx, own, targets), BF16),
            pltpu.VMEM((nt, own, targets), BF16),
            pltpu.VMEM((nt, own, targets), BF16),
            pltpu.VMEM((total, 1), jnp.int32),
            pltpu.SMEM(tile_pattern.shape, jnp.int32),
            sem(10),
            sem(1), sem(nt), sem(1), sem(1), sem(1), sem(nt),
            sem(1), sem(1), sem(nt, groups + repeat - 1), sem(1), sem(1), sem(nt),
            sem(1), sem(nt, nx), sem(1), sem(nt, nx),
            sem(1), sem(nx), sem(1), sem(nx),
            sem(1), sem(nt, nx), sem(1), sem(nt, nx), sem(1), sem(1),
        ],
        compiler_params=pltpu.CompilerParams(
            collective_id=0, has_side_effects=True, vmem_limit_bytes=60 * 1024 * 1024
        ),
    )(
        target_rows, target_pos.reshape(1, targets), decoder_rows, source_pos.reshape(1, total),
        out_proj, value_proj, attention, tile_pattern,
    )


def resident_bytes(nt, ns, width, heads, depth, groups, rows, total, targets):
    weights = heads * depth * 128 + groups * width * 128
    gathered = nt * ns * rows * depth + nt * heads * targets * 128
    return 2 * (weights + gathered) + 4 * nt * total * targets * 2


def shards(
    target_rows, target_pos, decoder_rows, source_pos, out_proj, value_proj, attention, tile_pattern
):
    nt, ns = lax.axis_size("tgt"), lax.axis_size("src")
    heads, depth, head_dim = out_proj.shape
    need = resident_bytes(
        nt, ns, target_rows.shape[1], heads, depth, value_proj.shape[0], target_rows.shape[0],
        source_pos.shape[0], target_pos.shape[0],
    )
    fits = (
        depth % 128 == 0 and head_dim == 128 and ns % 2 == 0 and nt > 2
        and decoder_rows.shape[0] % 16 == 0 and attention.shape[1] % 16 == 0
        and attention.shape[2] == 2 * head_dim and nt == 4
        and value_proj.shape[0] == 4 and heads == 8
        and 2 * heads * attention.shape[1] * nt <= target_rows.shape[1]
        and need < 40 * 1024 * 1024
    )
    plan = resident_shards if fits else gathered_shards
    return plan(
        target_rows, target_pos, decoder_rows, source_pos, out_proj, value_proj, attention, tile_pattern
    )


def solution(mesh):
    return jax.shard_map(
        shards,
        mesh=mesh,
        in_specs=(
            P(("grp", "tgt", "src"), None),
            P(("grp", "tgt")),
            P(("grp", "tgt", "src"), None),
            P("grp"),
            P("src", "tgt", None),
            P("src", None, None),
            P(("grp", "src"), "tgt", None),
            P("grp", None),
        ),
        out_specs=P(("grp", "src"), "tgt"),
        check_vma=False,
    )
```

```python
import functools

import jax
import jax.numpy as jnp
from jax import lax
from jax.experimental import pallas as pl
from jax.experimental.pallas import tpu as pltpu
from jax.sharding import PartitionSpec as P


def passed_along(value, axis, steps):
    count = lax.axis_size(axis)
    pairs = [(source, (source + steps) % count) for source in range(count)]
    return lax.ppermute(value, axis, pairs)


def gathered_shards(
    target_rows, target_pos, decoder_rows, source_pos, out_proj, value_proj, attention, tile_pattern
):
    blocks = lax.axis_size("tgt")
    column = lax.axis_index("tgt")
    src_lane = lax.axis_index("src")
    full_targets, full_sources = (
        lax.all_gather(target_rows, "src", axis=0, tiled=True),
        lax.all_gather(decoder_rows, "src", axis=0, tiled=True),
    )
    tgt_dev = full_targets.shape[0]
    src_dev = full_sources.shape[0]
    sub_rows = decoder_rows.shape[0]
    heads_here = out_proj.shape[0]
    head_dim = out_proj.shape[2]
    groups_here = value_proj.shape[0]
    repeat = heads_here // groups_here
    read_sum = jnp.einsum(
        "td,hde->the",
        full_targets,
        lax.all_gather(out_proj, "tgt", axis=1, tiled=True),
        preferred_element_type=jnp.float32,
    )
    head_reads = read_sum.astype(jnp.bfloat16).reshape(tgt_dev, groups_here, repeat, head_dim)
    values = jnp.einsum("sd,gde->sge", full_sources, value_proj, preferred_element_type=jnp.float32)
    values = values.astype(jnp.bfloat16).reshape(src_dev, groups_here * head_dim)
    attn_table = lax.all_gather(attention, "tgt", axis=1, tiled=True)
    target_attn = jnp.take(attn_table, target_pos, axis=1)
    keyed_attn = jnp.transpose(target_attn, (0, 2, 1))

    def edge_tile(payload, block_index):
        decoder_part, value_part = payload
        key_positions = lax.dynamic_slice_in_dim(source_pos, block_index * src_dev, src_dev)
        weights = jnp.take(keyed_attn, key_positions, axis=1).astype(jnp.float32)
        scores = jnp.einsum(
            "sgd,tgrd->grst",
            value_part.reshape(src_dev, groups_here, head_dim),
            head_reads,
            preferred_element_type=jnp.float32,
        )
        scores = scores.reshape(heads_here, src_dev, tgt_dev)
        mixed_term = jnp.sum(weights * scores, axis=0)
        own_positions = lax.dynamic_slice_in_dim(key_positions, src_lane * sub_rows, sub_rows)
        same_place = (own_positions[:, None] == target_pos[None, :]).astype(jnp.float32)
        direct = (
            jnp.einsum("sd,td->st", decoder_part, full_targets, preferred_element_type=jnp.float32)
            * same_place
        )
        own_rows = lax.dynamic_slice_in_dim(mixed_term, src_lane * sub_rows, sub_rows, 0)
        return lax.dynamic_update_slice_in_dim(
            mixed_term, own_rows + direct, src_lane * sub_rows, 0
        )

    def place_tile(partial_value, payload, block_index):
        kept_flag = tile_pattern[block_index, column]
        piece_tile = edge_tile(payload, block_index) * kept_flag.astype(jnp.float32)
        return lax.dynamic_update_slice_in_dim(partial_value, piece_tile, block_index * src_dev, 0)

    own_block = (decoder_rows, values)
    partial_value = jnp.zeros((blocks * src_dev, tgt_dev), jnp.float32)
    partial_value = place_tile(partial_value, own_block, column)

    def cycle_turn(turn_index, state_carry):
        forward_block, backward_block, running = state_carry
        forward_block = passed_along((forward_block[0], forward_block[1]), "tgt", 1)
        backward_block = passed_along((backward_block[0], backward_block[1]), "tgt", -1)
        running = place_tile(running, forward_block, (column - turn_index) % blocks)
        running = place_tile(running, backward_block, (column + turn_index) % blocks)
        return (forward_block, backward_block, running)

    forward_block, backward_block, partial_value = lax.fori_loop(
        1, blocks // 2, cycle_turn, (own_block, own_block, partial_value)
    )
    forward_block = passed_along((forward_block[0], forward_block[1]), "tgt", 1)
    partial_value = place_tile(partial_value, forward_block, (column - blocks // 2) % blocks)
    summed = lax.psum_scatter(partial_value, "src", scatter_dimension=0, tiled=True)
    return summed.astype(jnp.bfloat16)


F32 = jnp.float32
BF16 = jnp.bfloat16
MESH = pl.DeviceIdType.MESH


def dot(a, b):
    return jnp.dot(a, b, preferred_element_type=F32)


def dot_nt(a, b):
    return lax.dot_general(a, b, (((1,), (1,)), ((), ())), preferred_element_type=F32)


def edge_kernel(
    nt, ns, tgt_hbm, tpos_hbm, dec_hbm, srow_hbm, oproj_hbm, vproj_hbm, attn_hbm, pat_hbm,
    out_ref,
    oproj, vproj, tslices, dslices, decfull, attn, packs, tpos, srow, values, reads, pick, attn_n, onehot,
    edges, core_in, x_out, x_in, z_out, z_in, scol_ref, pat_ref,
    local_sem, zt_s, zt_r, zd_s, zd_r, zp_s, zp_r, ar_s, al_s, a_r, vr_s, vl_s, v_r,
    xt_s, xt_r, ct_s, ct_r, xf_s, xf_r, cf_s, cf_r, ce_s, ce_r, xe_s, xe_r, ze_s, ze_r,
):
    c = lax.axis_index("tgt")
    s = lax.axis_index("src")
    nx = ns // 2
    x = s // 2
    core = s % 2
    mate = x * 2 + 1 - core
    rows, depth = tslices.shape[1] // ns, tslices.shape[2]
    sub = dec_hbm.shape[0]
    heads = oproj.shape[0]
    groups = vproj.shape[0]
    repeat = heads // groups
    block = sub * ns
    queries, keys = attn_hbm.shape[1:]
    targets = tpos.shape[2]
    total = scol_ref.shape[0]
    own = edges.shape[1] // ns
    hd = vproj.shape[2]

    inner = (c > 0) & (c + 1 < nt)

    def table(rank):
        rows_of = [[i] + sorted((b for b in range(nt) if b != i), key=lambda b: rank(i, b)) for i in range(nt)]

        def entry(j):
            b = rows_of[0][j]
            for i in range(1, nt):
                b = jnp.where(c == i, rows_of[i][j], b)
            return b

        return [entry(j) for j in range(nt)]

    def sent_rank(i, b):
        return abs(b - i) if 0 < i < nt - 1 else -abs(b - i)

    def got_rank(i, b):
        far = abs(b - i)
        return (-far, b in (0, nt - 1)) if 0 < i < nt - 1 else (b in (0, nt - 1) and -far, far)

    targets_of = table(sent_rank)
    order = table(got_rank)
    last_of = table(lambda i, b: -b)

    def xsrc(dx):
        return lax.rem(x + dx, nx) * 2 + core

    def remote(src, dst, ssem, rsem, axis, index):
        return pltpu.make_async_remote_copy(
            src_ref=src, dst_ref=dst, send_sem=ssem, recv_sem=rsem,
            device_id={axis: index}, device_id_type=MESH,
        )

    def send(src, dst, ssem, rsem, axis, index):
        remote(src, dst, ssem, rsem, axis, index).start()

    def arrived(dst, rsem):
        remote(dst, dst, local_sem.at[0], rsem, "src", mate).wait_recv()

    barrier = pltpu.get_barrier_semaphore()
    for j in range(1, nt):
        pl.semaphore_signal(barrier, inc=1, device_id={"tgt": order[j]}, device_id_type=MESH)
    for dx in range(1, nx):
        pl.semaphore_signal(barrier, inc=1, device_id={"src": xsrc(dx)}, device_id_type=MESH)
    pl.semaphore_signal(barrier, inc=1, device_id={"src": mate}, device_id_type=MESH)

    def cols(b):
        return pl.ds(pl.multiple_of(b * depth, 128), depth)

    def trow(lane):
        return pl.ds(pl.multiple_of(lane * rows, rows), rows)

    def drow(lane):
        return pl.ds(pl.multiple_of(lane * sub, sub), sub)

    def qrow(b):
        return pl.ds(pl.multiple_of(b * queries, queries), queries)

    def vrow(b):
        return pl.ds(pl.multiple_of(b * block, block), block)

    def erow(lane):
        return pl.ds(pl.multiple_of(lane * own, own), own)

    fetch = [
        pltpu.make_async_copy(dec_hbm, decfull.at[drow(s)], local_sem.at[1]),
        pltpu.make_async_copy(srow_hbm, srow, local_sem.at[2]),
        pltpu.make_async_copy(tpos_hbm, tpos.at[c], local_sem.at[3]),
        pltpu.make_async_copy(vproj_hbm, vproj, local_sem.at[4]),
        pltpu.make_async_copy(tgt_hbm.at[:, cols(c)], tslices.at[c, trow(s)], local_sem.at[5]),
        pltpu.make_async_copy(dec_hbm.at[:, cols(c)], dslices.at[drow(c)], local_sem.at[6]),
        pltpu.make_async_copy(oproj_hbm, oproj, local_sem.at[7]),
        pltpu.make_async_copy(attn_hbm, attn.at[:, qrow(c), :], local_sem.at[8]),
        pltpu.make_async_copy(pat_hbm, pat_ref, local_sem.at[9]),
    ]
    for cp in fetch[:7] + fetch[8:]:
        cp.start()
    pl.semaphore_wait(barrier, nt - 1 + nx)

    chunks = [(g * repeat, repeat) for g in range(groups - 1)]
    chunks += [(heads - repeat + r, 1) for r in range(repeat)]
    half = keys // 2
    lowest = half // queries if half % 128 == 0 else 0
    packed = nt - 2
    if repeat != 2 or packed < lowest or lowest == 0 or (packed + 1) * queries - half != half // 2:
        packed = -1

    def attn_copy(b, g, ssem, device, act, src=None):
        part = pl.ds(*chunks[g])

        def view(lanes):
            dst = attn.at[part, qrow(b), lanes]
            return dst if src is None else src.at[part, :, lanes], dst

        @pl.when(b < lowest)
        def _():
            a, d = view(pl.ds(0, half))
            act(remote(a, d, ssem.at[0], a_r.at[b, g], "tgt", device))

        if packed >= 0 and g < groups:
            @pl.when(b == packed)
            def _():
                act(remote(packs.at[g], packs.at[g], ssem.at[0], a_r.at[b, g], "tgt", device))

        @pl.when((b >= lowest) & (b != packed))
        def _():
            a, d = view(pl.ds(0, keys))
            act(remote(a, d, ssem.at[0], a_r.at[b, g], "tgt", device))

    def value_copy(b, ssem, device):
        dst = values.at[:, vrow(b), :]
        return remote(dst, dst, ssem.at[0], v_r.at[b], "tgt", device)

    start = lambda copy: copy.start()
    wait_send = lambda copy: copy.wait_send()
    wait_recv = lambda copy: copy.wait_recv()

    def rightward(act):
        pl.when(c + 1 < nt)(act)

    def leftward(act):
        pl.when(c > 0)(act)

    for dx in range(1, nx):
        send(dec_hbm, decfull.at[drow(s)], xf_s.at[0], xf_r.at[x], "src", xsrc(dx))
    send(dec_hbm, decfull.at[drow(s)], cf_s.at[0], cf_r.at[0], "src", mate)
    def spread_copies(b):
        return (
            remote(tgt_hbm.at[:, cols(b)], tslices.at[c, trow(s)], zt_s.at[0], zt_r.at[c], "tgt", b),
            remote(tpos_hbm, tpos.at[c], zp_s.at[0], zp_r.at[c], "tgt", b),
        )

    def slice_copy(b):
        return remote(dec_hbm.at[:, cols(b)], dslices.at[drow(c)], zd_s.at[0], zd_r.at[0], "tgt", b)

    def send_slices():
        for j in range(1, nt):
            slice_copy(targets_of[j]).start()

    def spread(j):
        b = targets_of[j]
        for copy in spread_copies(b):
            copy.start()

    spread(1)
    spread(2)
    for dx in range(1, nx):
        send(tgt_hbm.at[:, cols(c)], tslices.at[c, trow(s)], xt_s.at[0], xt_r.at[c, x], "src", xsrc(dx))
    send(tgt_hbm.at[:, cols(c)], tslices.at[c, trow(s)], ct_s.at[0], ct_r.at[c], "src", mate)

    fetch[1].wait()
    fetch[2].wait()
    scol_ref[...] = jnp.transpose(jnp.broadcast_to(srow[...], (128, total)))[:, :1]
    pick[...] = (scol_ref[...] == lax.broadcasted_iota(jnp.int32, (total, keys), 1)).astype(BF16)
    for b in range(lowest):
        attn[:, b * queries:(b + 1) * queries, half:] = jnp.zeros((heads, queries, keys - half), BF16)
    fetch[7].start()

    def relay(k, copy_in, copy_on):
        @pl.when(c - k >= 0)
        def _():
            copy_in(c - k)
            rightward(lambda: copy_on(c - k, 0))

        @pl.when(c + k < nt)
        def _():
            copy_in(c + k)
            leftward(lambda: copy_on(c + k, 1))

    def attn_step(k, g):
        relay(
            k, lambda b: attn_copy(b, g, ar_s, c, wait_recv),
            lambda b, left: attn_copy(b, g, al_s if left else ar_s, c - 1 if left else c + 1, start),
        )

    def value_step(k):
        relay(
            k, lambda b: value_copy(b, vr_s, c).wait_recv(),
            lambda b, left: value_copy(b, vl_s if left else vr_s, c - 1 if left else c + 1).start(),
        )

    def take(j):
        b = order[j]
        arrived(tslices.at[b, trow(s)], zt_r.at[b])
        for dx in range(1, nx):
            send(tslices.at[b, trow(s)], tslices.at[b, trow(s)], xt_s.at[0], xt_r.at[b, x], "src", xsrc(dx))
        send(tslices.at[b, trow(s)], tslices.at[b, trow(s)], ct_s.at[0], ct_r.at[b], "src", mate)

    fetch[0].wait()
    for dx in range(1, nx):
        z = lax.rem(x + dx, nx)
        y = xsrc(dx)
        arrived(decfull.at[drow(y)], xf_r.at[z])
        send(decfull.at[drow(y)], decfull.at[drow(y)], cf_s.at[0], cf_r.at[0], "src", mate)
    arrived(decfull.at[:nx * sub], cf_r.at[0])
    fetch[3].wait()

    @pl.loop(0, groups)
    def _(g):
        values[g, vrow(c)] = dot(decfull[...], vproj[g]).astype(BF16)

    fetch[7].wait()
    if packed >= 0:
        @pl.when(c == packed)
        def _():
            at = slice(packed * queries, (packed + 1) * queries)
            for g in range(groups):
                packs[g, 0] = attn[2 * g, at, :half]
                packs[g, 1] = attn[2 * g + 1, at, :half]
                packs[g, 2] = jnp.concatenate(
                    [attn[2 * g + r, at, half:half + half // 2] for r in range(2)], axis=1
                )
    rightward(lambda: value_copy(c, vr_s, c + 1).start())
    leftward(lambda: value_copy(c, vl_s, c - 1).start())

    def cross(j):
        b = order[j]
        for dx in range(1, nx):
            z = lax.rem(x + dx, nx)
            y = z * 2 + core
            arrived(tslices.at[b, trow(y)], xt_r.at[b, z])
            send(tslices.at[b, trow(y)], tslices.at[b, trow(y)], ct_s.at[0], ct_r.at[b], "src", mate)

    def ready(j):
        b = order[j]
        if j == 0:
            fetch[4].wait()
            fetch[6].wait()
        else:
            arrived(tpos.at[b], zp_r.at[b])
        arrived(tslices.at[b, :nx * rows], ct_r.at[b])

    def read_block(j, part):
        b = order[j]
        share = groups // 2

        @pl.loop(part * share, groups if part else share)
        def _(g):
            pair = jnp.concatenate([oproj[g * repeat + r] for r in range(repeat)], axis=1)
            reads[b, g] = dot(tslices[b], pair).astype(BF16)

        if part:
            onehot[b] = (
                lax.broadcasted_iota(jnp.int32, (nt * queries, targets), 0) == tpos[b]
            ).astype(BF16)

    def wait_slices():
        fetch[5].wait()
        arrived(dslices.at[:(nt - 1) * sub], zd_r.at[0])

    def add_direct(b):
        direct = dot_nt(dslices[...], tslices[b])
        here = tpos[b]
        for p in range(nt):
            at = pl.ds(pl.multiple_of(p * block + s * sub, sub), sub)
            same = (scol_ref[at] == here).astype(F32)
            edges[b, at] += direct[p * sub:(p + 1) * sub] * same

    def unpack(g):
        at = slice(packed * queries, (packed + 1) * queries)
        both = packs[g, 2].astype(F32)
        lane = lax.broadcasted_iota(jnp.int32, both.shape, 1)
        for r in range(2):
            attn[2 * g + r, at, :half] = packs[g, r]
            upper = pltpu.roll(both, half // 2, 1) if r else both
            attn[2 * g + r, at, half:] = jnp.where(lane < half // 2, upper, 0.0).astype(BF16)

    def pick_keys(i):
        if packed >= 0 and i < groups:
            pl.when(c != packed)(lambda: unpack(i))
        for h in range(chunks[i][0], sum(chunks[i])):
            attn_n[h] = dot_nt(pick[...], attn[h]).astype(BF16)

    def issue(g):
        rightward(lambda: attn_copy(c, g, ar_s, c + 1, start, attn_hbm))
        leftward(lambda: attn_copy(c, g, al_s, c - 1, start, attn_hbm))

    def mix_all(g):
        for j in range(nt):
            mix(g, last_of[j])

    def add_all():
        for j in range(nt):
            add_direct(last_of[j])

    def mix(i, b):
        terms = None
        for h in range(chunks[i][0], sum(chunks[i])):
            g, r = h // repeat, h % repeat
            term = dot(attn_n[h], onehot[b]) * dot_nt(values[g], reads[b, g, :, r * hd:(r + 1) * hd])
            terms = term if terms is None else terms + term
        edges[b] = terms if i == 0 else edges[b] + terms

    def to_mate(b):
        for z in range(nx):
            send(edges.at[b, erow(z * 2 + 1 - core)], core_in.at[b, z], ce_s.at[0], ce_r.at[b], "src", mate)

    def over_x(b):
        arrived(core_in.at[b], ce_r.at[b])
        for dx in range(1, nx):
            z = lax.rem(x + dx, nx)
            x_out[b, z] = (edges[b, erow(z * 2 + core)] + core_in[b, z]).astype(BF16)
            send(x_out.at[b, z], x_in.at[b, x], xe_s.at[0], xe_r.at[b, x], "src", z * 2 + core)

    def over_z(b, away):
        mine = edges[b, erow(s)] + core_in[b, x]
        for dx in range(1, nx):
            z = lax.rem(x + dx, nx)
            arrived(x_in.at[b, z], xe_r.at[b, z])
            mine += x_in[b, z].astype(F32)
        if away:
            z_out[b] = mine.astype(BF16)
            send(z_out.at[b], z_in.at[c], ze_s.at[0], ze_r.at[0], "tgt", b)
        return mine

    spread(3)
    issue(0)
    take(1)
    issue(1)
    take(2)
    cross(0)
    issue(2)
    cross(1)
    value_step(1)
    ready(0)
    take(3)
    issue(3)
    ready(1)
    read_block(0, 1)
    read_block(1, 0)
    attn_step(1, 0)
    issue(4)
    read_block(0, 0)
    attn_step(1, 1)
    read_block(1, 1)
    attn_step(1, 2)
    value_step(2)
    attn_step(1, 3)
    cross(2)
    ready(2)
    attn_step(2, 0)
    read_block(2, 1)
    pl.when(jnp.logical_not(inner))(send_slices)
    pl.when(inner)(send_slices)
    cross(3)
    value_step(3)
    attn_step(2, 1)
    attn_step(1, 4)
    read_block(2, 0)
    ready(3)
    read_block(3, 1)
    attn_step(3, 0)
    pick_keys(0)
    read_block(3, 0)
    mix_all(0)
    attn_step(2, 2)
    attn_step(3, 1)
    pick_keys(1)
    attn_step(2, 3)
    mix_all(1)
    wait_slices()
    add_all()
    attn_step(3, 2)
    pick_keys(2)
    mix_all(2)
    attn_step(2, 4)
    attn_step(3, 3)
    pick_keys(3)
    mix_all(3)
    attn_step(3, 4)
    last = len(chunks) - 1
    pick_keys(last)
    mix(last, last_of[1])
    to_mate(last_of[1])
    mix(last, last_of[2])
    to_mate(last_of[2])
    for j in range(3, nt):
        mix(last, last_of[j])
        to_mate(last_of[j])
        over_x(last_of[j - 2])
    mix(last, c)
    to_mate(c)
    over_x(last_of[nt - 2])
    over_x(last_of[nt - 1])
    over_x(c)
    for j in range(1, nt):
        over_z(last_of[j], True)
    mine = over_z(c, False)
    fetch[8].wait()
    def drained(view, ssem):
        remote(view, view, ssem.at[0], local_sem.at[0], "src", mate).wait_send()

    drained(tslices.at[:nt - 1, :rows], zt_s)
    drained(tslices.at[:, :(nx - 1) * rows], xt_s)
    drained(tslices.at[:, :nx * rows], ct_s)
    drained(dslices.at[:(nt - 1) * sub], zd_s)
    drained(tpos.at[:nt - 1], zp_s)
    drained(decfull.at[:(nx - 1) * sub], xf_s)
    drained(decfull.at[:nx * sub], cf_s)
    drained(core_in, ce_s)
    drained(x_out.at[:, :nx - 1], xe_s)
    drained(z_out.at[:nt - 1], ze_s)

    def tiles(b):
        return heads if b < lowest else 3 * groups if b == packed else 2 * heads

    for i in range(nt):
        @pl.when(c == i)
        def _():
            if i + 1 < nt:
                drained(vproj.at[0, :queries * sum(tiles(b) for b in range(i + 1))], ar_s)
                drained(values.at[:, :(i + 1) * block], vr_s)
            if i > 0:
                drained(vproj.at[0, :queries * sum(tiles(b) for b in range(i, nt))], al_s)
                drained(values.at[:, :(nt - i) * block], vl_s)

    arrived(z_in.at[:nt - 1], ze_r.at[0])
    for j in range(1, nt):
        mine += z_in[order[j]].astype(F32)
    kept = pat_ref[(s * own) // block, c]
    out_ref[...] = (mine * kept.astype(F32)).astype(BF16)


def resident_shards(
    target_rows, target_pos, decoder_rows, source_pos, out_proj, value_proj, attention, tile_pattern
):
    nt, ns = lax.axis_size("tgt"), lax.axis_size("src")
    rows = target_rows.shape[0]
    sub, width = decoder_rows.shape
    heads, depth, head_dim = out_proj.shape
    groups = value_proj.shape[0]
    repeat = heads // groups
    _, queries, keys = attention.shape
    total = source_pos.shape[0]
    targets = target_pos.shape[0]
    own = total // ns
    nx = ns // 2
    vmem = pl.BlockSpec(memory_space=pltpu.VMEM)
    hbm = pl.BlockSpec(memory_space=pl.ANY)
    sem = lambda *shape: pltpu.SemaphoreType.DMA(shape)
    return pl.pallas_call(
        functools.partial(edge_kernel, nt, ns),
        out_shape=pltpu.VMEM((own, targets), BF16),
        in_specs=[hbm] * 8,
        out_specs=vmem,
        scratch_shapes=[
            pltpu.VMEM(out_proj.shape, BF16),
            pltpu.VMEM(value_proj.shape, BF16),
            pltpu.VMEM((nt, ns * rows, depth), BF16),
            pltpu.VMEM((nt * sub, depth), BF16),
            pltpu.VMEM((ns * sub, width), BF16),
            pltpu.VMEM((heads, nt * queries, keys), BF16),
            pltpu.VMEM((groups, 3, queries, keys // 2), BF16),
            pltpu.VMEM((nt, 1, targets), jnp.int32),
            pltpu.VMEM((1, total), jnp.int32),
            pltpu.VMEM((groups, total, head_dim), BF16),
            pltpu.VMEM((nt, groups, targets, repeat * head_dim), BF16),
            pltpu.VMEM((total, keys), BF16),
            pltpu.VMEM((heads, total, nt * queries), BF16),
            pltpu.VMEM((nt, nt * queries, targets), BF16),
            pltpu.VMEM((nt, total, targets), F32),
            pltpu.VMEM((nt, nx, own, targets), F32),
            pltpu.VMEM((nt, nx, own, targets), BF16),
            pltpu.VMEM((nt, nx, own, targets), BF16),
            pltpu.VMEM((nt, own, targets), BF16),
            pltpu.VMEM((nt, own, targets), BF16),
            pltpu.VMEM((total, 1), jnp.int32),
            pltpu.SMEM(tile_pattern.shape, jnp.int32),
            sem(10),
            sem(1), sem(nt), sem(1), sem(1), sem(1), sem(nt),
            sem(1), sem(1), sem(nt, groups + repeat - 1), sem(1), sem(1), sem(nt),
            sem(1), sem(nt, nx), sem(1), sem(nt),
            sem(1), sem(nx), sem(1), sem(1),
            sem(1), sem(nt), sem(1), sem(nt, nx), sem(1), sem(1),
        ],
        compiler_params=pltpu.CompilerParams(
            collective_id=0, has_side_effects=True, vmem_limit_bytes=60 * 1024 * 1024
        ),
    )(
        target_rows, target_pos.reshape(1, targets), decoder_rows, source_pos.reshape(1, total),
        out_proj, value_proj, attention, tile_pattern,
    )


def resident_bytes(nt, ns, width, heads, depth, groups, rows, total, targets):
    weights = heads * depth * 128 + groups * width * 128
    gathered = nt * ns * rows * depth + nt * heads * targets * 128
    return 2 * (weights + gathered) + 4 * nt * total * targets * 2


def shards(
    target_rows, target_pos, decoder_rows, source_pos, out_proj, value_proj, attention, tile_pattern
):
    nt, ns = lax.axis_size("tgt"), lax.axis_size("src")
    heads, depth, head_dim = out_proj.shape
    need = resident_bytes(
        nt, ns, target_rows.shape[1], heads, depth, value_proj.shape[0], target_rows.shape[0],
        source_pos.shape[0], target_pos.shape[0],
    )
    fits = (
        depth % 128 == 0 and head_dim == 128 and ns % 2 == 0 and nt > 2
        and decoder_rows.shape[0] % 16 == 0 and attention.shape[1] % 16 == 0
        and attention.shape[2] == 2 * head_dim and nt == 4
        and value_proj.shape[0] == 4 and heads == 8
        and 2 * heads * attention.shape[1] * nt <= target_rows.shape[1]
        and need < 40 * 1024 * 1024
    )
    plan = resident_shards if fits else gathered_shards
    return plan(
        target_rows, target_pos, decoder_rows, source_pos, out_proj, value_proj, attention, tile_pattern
    )


def solution(mesh):
    return jax.shard_map(
        shards,
        mesh=mesh,
        in_specs=(
            P(("grp", "tgt", "src"), None),
            P(("grp", "tgt")),
            P(("grp", "tgt", "src"), None),
            P("grp"),
            P("src", "tgt", None),
            P("src", None, None),
            P(("grp", "src"), "tgt", None),
            P("grp", None),
        ),
        out_specs=P(("grp", "src"), "tgt"),
        check_vma=False,
    )
```

```python
import functools

import jax
import jax.numpy as jnp
from jax import lax
from jax.experimental import pallas as pl
from jax.experimental.pallas import tpu as pltpu
from jax.sharding import PartitionSpec as P


def passed_along(value, axis, steps):
    count = lax.axis_size(axis)
    pairs = [(source, (source + steps) % count) for source in range(count)]
    return lax.ppermute(value, axis, pairs)


def gathered_shards(
    target_rows, target_pos, decoder_rows, source_pos, out_proj, value_proj, attention, tile_pattern
):
    blocks = lax.axis_size("tgt")
    column = lax.axis_index("tgt")
    src_lane = lax.axis_index("src")
    full_targets, full_sources = (
        lax.all_gather(target_rows, "src", axis=0, tiled=True),
        lax.all_gather(decoder_rows, "src", axis=0, tiled=True),
    )
    tgt_dev = full_targets.shape[0]
    src_dev = full_sources.shape[0]
    sub_rows = decoder_rows.shape[0]
    heads_here = out_proj.shape[0]
    head_dim = out_proj.shape[2]
    groups_here = value_proj.shape[0]
    repeat = heads_here // groups_here
    read_sum = jnp.einsum(
        "td,hde->the",
        full_targets,
        lax.all_gather(out_proj, "tgt", axis=1, tiled=True),
        preferred_element_type=jnp.float32,
    )
    head_reads = read_sum.astype(jnp.bfloat16).reshape(tgt_dev, groups_here, repeat, head_dim)
    values = jnp.einsum("sd,gde->sge", full_sources, value_proj, preferred_element_type=jnp.float32)
    values = values.astype(jnp.bfloat16).reshape(src_dev, groups_here * head_dim)
    attn_table = lax.all_gather(attention, "tgt", axis=1, tiled=True)
    target_attn = jnp.take(attn_table, target_pos, axis=1)
    keyed_attn = jnp.transpose(target_attn, (0, 2, 1))

    def edge_tile(payload, block_index):
        decoder_part, value_part = payload
        key_positions = lax.dynamic_slice_in_dim(source_pos, block_index * src_dev, src_dev)
        weights = jnp.take(keyed_attn, key_positions, axis=1).astype(jnp.float32)
        scores = jnp.einsum(
            "sgd,tgrd->grst",
            value_part.reshape(src_dev, groups_here, head_dim),
            head_reads,
            preferred_element_type=jnp.float32,
        )
        scores = scores.reshape(heads_here, src_dev, tgt_dev)
        mixed_term = jnp.sum(weights * scores, axis=0)
        own_positions = lax.dynamic_slice_in_dim(key_positions, src_lane * sub_rows, sub_rows)
        same_place = (own_positions[:, None] == target_pos[None, :]).astype(jnp.float32)
        direct = (
            jnp.einsum("sd,td->st", decoder_part, full_targets, preferred_element_type=jnp.float32)
            * same_place
        )
        own_rows = lax.dynamic_slice_in_dim(mixed_term, src_lane * sub_rows, sub_rows, 0)
        return lax.dynamic_update_slice_in_dim(
            mixed_term, own_rows + direct, src_lane * sub_rows, 0
        )

    def place_tile(partial_value, payload, block_index):
        kept_flag = tile_pattern[block_index, column]
        piece_tile = edge_tile(payload, block_index) * kept_flag.astype(jnp.float32)
        return lax.dynamic_update_slice_in_dim(partial_value, piece_tile, block_index * src_dev, 0)

    own_block = (decoder_rows, values)
    partial_value = jnp.zeros((blocks * src_dev, tgt_dev), jnp.float32)
    partial_value = place_tile(partial_value, own_block, column)

    def cycle_turn(turn_index, state_carry):
        forward_block, backward_block, running = state_carry
        forward_block = passed_along((forward_block[0], forward_block[1]), "tgt", 1)
        backward_block = passed_along((backward_block[0], backward_block[1]), "tgt", -1)
        running = place_tile(running, forward_block, (column - turn_index) % blocks)
        running = place_tile(running, backward_block, (column + turn_index) % blocks)
        return (forward_block, backward_block, running)

    forward_block, backward_block, partial_value = lax.fori_loop(
        1, blocks // 2, cycle_turn, (own_block, own_block, partial_value)
    )
    forward_block = passed_along((forward_block[0], forward_block[1]), "tgt", 1)
    partial_value = place_tile(partial_value, forward_block, (column - blocks // 2) % blocks)
    summed = lax.psum_scatter(partial_value, "src", scatter_dimension=0, tiled=True)
    return summed.astype(jnp.bfloat16)


F32 = jnp.float32
BF16 = jnp.bfloat16
MESH = pl.DeviceIdType.MESH


def dot(a, b):
    return jnp.dot(a, b, preferred_element_type=F32)


def dot_nt(a, b):
    return lax.dot_general(a, b, (((1,), (1,)), ((), ())), preferred_element_type=F32)


def edge_kernel(
    nt, ns, tgt_hbm, tpos_hbm, dec_hbm, srow_hbm, oproj_hbm, vproj_hbm, attn_hbm, pat_hbm,
    out_ref,
    oproj, vproj, tslices, dslices, decfull, attn, packs, tpos, srow, values, reads, pick, attn_n, onehot,
    edges, core_in, x_out, x_in, z_out, z_in, scol_ref, pat_ref,
    local_sem, zt_s, zt_r, zd_s, zd_r, zp_s, zp_r, ar_s, al_s, a_r, vr_s, vl_s, v_r,
    xt_s, xt_r, ct_s, ct_r, xf_s, xf_r, cf_s, cf_r, ce_s, ce_r, xe_s, xe_r, ze_s, ze_r,
):
    c = lax.axis_index("tgt")
    s = lax.axis_index("src")
    nx = ns // 2
    x = s // 2
    core = s % 2
    mate = x * 2 + 1 - core
    rows, depth = tslices.shape[1] // ns, tslices.shape[2]
    sub = dec_hbm.shape[0]
    heads = oproj.shape[0]
    groups = vproj.shape[0]
    repeat = heads // groups
    block = sub * ns
    queries, keys = attn_hbm.shape[1:]
    targets = tpos.shape[2]
    total = scol_ref.shape[0]
    own = edges.shape[1] // ns
    hd = vproj.shape[2]

    inner = (c > 0) & (c + 1 < nt)

    def table(rank):
        rows_of = [[i] + sorted((b for b in range(nt) if b != i), key=lambda b: rank(i, b)) for i in range(nt)]

        def entry(j):
            b = rows_of[0][j]
            for i in range(1, nt):
                b = jnp.where(c == i, rows_of[i][j], b)
            return b

        return [entry(j) for j in range(nt)]

    def sent_rank(i, b):
        return abs(b - i) if 0 < i < nt - 1 else -abs(b - i)

    def got_rank(i, b):
        far = abs(b - i)
        return (-far, b in (0, nt - 1)) if 0 < i < nt - 1 else (b in (0, nt - 1) and -far, far)

    targets_of = table(sent_rank)
    order = table(got_rank)
    last_of = table(lambda i, b: -b)

    def xsrc(dx):
        return lax.rem(x + dx, nx) * 2 + core

    def remote(src, dst, ssem, rsem, axis, index):
        return pltpu.make_async_remote_copy(
            src_ref=src, dst_ref=dst, send_sem=ssem, recv_sem=rsem,
            device_id={axis: index}, device_id_type=MESH,
        )

    def send(src, dst, ssem, rsem, axis, index):
        remote(src, dst, ssem, rsem, axis, index).start()

    def arrived(dst, rsem):
        remote(dst, dst, local_sem.at[0], rsem, "src", mate).wait_recv()

    barrier = pltpu.get_barrier_semaphore()
    for j in range(1, nt):
        pl.semaphore_signal(barrier, inc=1, device_id={"tgt": order[j]}, device_id_type=MESH)
    for dx in range(1, nx):
        pl.semaphore_signal(barrier, inc=1, device_id={"src": xsrc(dx)}, device_id_type=MESH)
    pl.semaphore_signal(barrier, inc=1, device_id={"src": mate}, device_id_type=MESH)

    def cols(b):
        return pl.ds(pl.multiple_of(b * depth, 128), depth)

    def trow(lane):
        return pl.ds(pl.multiple_of(lane * rows, rows), rows)

    def drow(lane):
        return pl.ds(pl.multiple_of(lane * sub, sub), sub)

    def qrow(b):
        return pl.ds(pl.multiple_of(b * queries, queries), queries)

    def vrow(b):
        return pl.ds(pl.multiple_of(b * block, block), block)

    def erow(lane):
        return pl.ds(pl.multiple_of(lane * own, own), own)

    fetch = [
        pltpu.make_async_copy(dec_hbm, decfull.at[drow(s)], local_sem.at[1]),
        pltpu.make_async_copy(srow_hbm, srow, local_sem.at[2]),
        pltpu.make_async_copy(tpos_hbm, tpos.at[c], local_sem.at[3]),
        pltpu.make_async_copy(vproj_hbm, vproj, local_sem.at[4]),
        pltpu.make_async_copy(tgt_hbm.at[:, cols(c)], tslices.at[c, trow(s)], local_sem.at[5]),
        pltpu.make_async_copy(dec_hbm.at[:, cols(c)], dslices.at[drow(c)], local_sem.at[6]),
        pltpu.make_async_copy(oproj_hbm, oproj, local_sem.at[7]),
        pltpu.make_async_copy(attn_hbm, attn.at[:, qrow(c), :], local_sem.at[8]),
        pltpu.make_async_copy(pat_hbm, pat_ref, local_sem.at[9]),
    ]
    for cp in fetch[:7] + fetch[8:]:
        cp.start()
    pl.semaphore_wait(barrier, nt - 1 + nx)

    chunks = [(g * repeat, repeat) for g in range(groups - 1)]
    chunks += [(heads - repeat + r, 1) for r in range(repeat)]
    half = keys // 2
    lowest = half // queries if half % 128 == 0 else 0
    packed = nt - 2
    if repeat != 2 or packed < lowest or lowest == 0 or (packed + 1) * queries - half != half // 2:
        packed = -1

    def attn_copy(b, g, ssem, device, act, src=None):
        part = pl.ds(*chunks[g])

        def view(lanes):
            dst = attn.at[part, qrow(b), lanes]
            return dst if src is None else src.at[part, :, lanes], dst

        @pl.when(b < lowest)
        def _():
            a, d = view(pl.ds(0, half))
            act(remote(a, d, ssem.at[0], a_r.at[b, g], "tgt", device))

        if packed >= 0 and g < groups:
            @pl.when(b == packed)
            def _():
                act(remote(packs.at[g], packs.at[g], ssem.at[0], a_r.at[b, g], "tgt", device))

        @pl.when((b >= lowest) & (b != packed))
        def _():
            a, d = view(pl.ds(0, keys))
            act(remote(a, d, ssem.at[0], a_r.at[b, g], "tgt", device))

    def value_copy(b, ssem, device):
        dst = values.at[:, vrow(b), :]
        return remote(dst, dst, ssem.at[0], v_r.at[b], "tgt", device)

    start = lambda copy: copy.start()
    wait_send = lambda copy: copy.wait_send()
    wait_recv = lambda copy: copy.wait_recv()

    def rightward(act):
        pl.when(c + 1 < nt)(act)

    def leftward(act):
        pl.when(c > 0)(act)

    for dx in range(1, nx):
        send(dec_hbm, decfull.at[drow(s)], xf_s.at[0], xf_r.at[dx - 1], "src", xsrc(dx))
    send(dec_hbm, decfull.at[drow(s)], cf_s.at[0], cf_r.at[0], "src", mate)
    def spread_copies(b):
        return (
            remote(tgt_hbm.at[:, cols(b)], tslices.at[c, trow(s)], zt_s.at[0], zt_r.at[c], "tgt", b),
            remote(tpos_hbm, tpos.at[c], zp_s.at[0], zp_r.at[c], "tgt", b),
        )

    def slice_copy(b):
        return remote(dec_hbm.at[:, cols(b)], dslices.at[drow(c)], zd_s.at[0], zd_r.at[0], "tgt", b)

    def send_slices():
        for j in range(1, nt):
            slice_copy(targets_of[j]).start()

    def spread(j):
        b = targets_of[j]
        for copy in spread_copies(b):
            copy.start()

    spread(1)
    spread(2)
    for dx in range(1, nx):
        send(tgt_hbm.at[:, cols(c)], tslices.at[c, trow(s)], xt_s.at[0], xt_r.at[c, dx - 1], "src", xsrc(dx))
    send(tgt_hbm.at[:, cols(c)], tslices.at[c, trow(s)], ct_s.at[0], ct_r.at[c], "src", mate)

    fetch[1].wait()
    fetch[2].wait()
    scol_ref[...] = jnp.transpose(jnp.broadcast_to(srow[...], (128, total)))[:, :1]
    pick[...] = (scol_ref[...] == lax.broadcasted_iota(jnp.int32, (total, keys), 1)).astype(BF16)
    for b in range(lowest):
        attn[:, b * queries:(b + 1) * queries, half:] = jnp.zeros((heads, queries, keys - half), BF16)
    fetch[7].start()

    def relay(k, copy_in, copy_on):
        @pl.when(c - k >= 0)
        def _():
            copy_in(c - k)
            rightward(lambda: copy_on(c - k, 0))

        @pl.when(c + k < nt)
        def _():
            copy_in(c + k)
            leftward(lambda: copy_on(c + k, 1))

    def attn_step(k, g):
        relay(
            k, lambda b: attn_copy(b, g, ar_s, c, wait_recv),
            lambda b, left: attn_copy(b, g, al_s if left else ar_s, c - 1 if left else c + 1, start),
        )

    def value_step(k):
        relay(
            k, lambda b: value_copy(b, vr_s, c).wait_recv(),
            lambda b, left: value_copy(b, vl_s if left else vr_s, c - 1 if left else c + 1).start(),
        )

    def take(j):
        b = order[j]
        arrived(tslices.at[b, trow(s)], zt_r.at[b])
        for dx in range(1, nx):
            send(tslices.at[b, trow(s)], tslices.at[b, trow(s)], xt_s.at[0], xt_r.at[b, dx - 1], "src", xsrc(dx))
        send(tslices.at[b, trow(s)], tslices.at[b, trow(s)], ct_s.at[0], ct_r.at[b], "src", mate)

    fetch[0].wait()
    for dx in range(1, nx):
        z = lax.rem(x + dx, nx)
        y = xsrc(dx)
        arrived(decfull.at[drow(y)], xf_r.at[nx - 1 - dx])
        send(decfull.at[drow(y)], decfull.at[drow(y)], cf_s.at[0], cf_r.at[0], "src", mate)
    arrived(decfull.at[:nx * sub], cf_r.at[0])
    fetch[3].wait()

    @pl.loop(0, groups)
    def _(g):
        values[g, vrow(c)] = dot(decfull[...], vproj[g]).astype(BF16)

    fetch[7].wait()
    if packed >= 0:
        @pl.when(c == packed)
        def _():
            at = slice(packed * queries, (packed + 1) * queries)
            for g in range(groups):
                packs[g, 0] = attn[2 * g, at, :half]
                packs[g, 1] = attn[2 * g + 1, at, :half]
                packs[g, 2] = jnp.concatenate(
                    [attn[2 * g + r, at, half:half + half // 2] for r in range(2)], axis=1
                )
    rightward(lambda: value_copy(c, vr_s, c + 1).start())
    leftward(lambda: value_copy(c, vl_s, c - 1).start())

    def cross(j):
        b = order[j]
        for dx in range(1, nx):
            z = lax.rem(x + dx, nx)
            y = z * 2 + core
            arrived(tslices.at[b, trow(y)], xt_r.at[b, nx - 1 - dx])
            send(tslices.at[b, trow(y)], tslices.at[b, trow(y)], ct_s.at[0], ct_r.at[b], "src", mate)

    def ready(j):
        b = order[j]
        if j == 0:
            fetch[4].wait()
            fetch[6].wait()
        else:
            arrived(tpos.at[b], zp_r.at[b])
        arrived(tslices.at[b, :nx * rows], ct_r.at[b])

    def read_block(j, part):
        b = order[j]
        share = groups // 2

        @pl.loop(part * share, groups if part else share)
        def _(g):
            pair = jnp.concatenate([oproj[g * repeat + r] for r in range(repeat)], axis=1)
            reads[b, g] = dot(tslices[b], pair).astype(BF16)

        if part:
            onehot[b] = (
                lax.broadcasted_iota(jnp.int32, (nt * queries, targets), 0) == tpos[b]
            ).astype(BF16)

    def wait_slices():
        fetch[5].wait()
        arrived(dslices.at[:(nt - 1) * sub], zd_r.at[0])

    def add_direct(b):
        direct = dot_nt(dslices[...], tslices[b])
        here = tpos[b]
        for p in range(nt):
            at = pl.ds(pl.multiple_of(p * block + s * sub, sub), sub)
            same = (scol_ref[at] == here).astype(F32)
            edges[b, at] += direct[p * sub:(p + 1) * sub] * same

    def unpack(g):
        at = slice(packed * queries, (packed + 1) * queries)
        both = packs[g, 2].astype(F32)
        lane = lax.broadcasted_iota(jnp.int32, both.shape, 1)
        for r in range(2):
            attn[2 * g + r, at, :half] = packs[g, r]
            upper = pltpu.roll(both, half // 2, 1) if r else both
            attn[2 * g + r, at, half:] = jnp.where(lane < half // 2, upper, 0.0).astype(BF16)

    def pick_keys(i):
        if packed >= 0 and i < groups:
            pl.when(c != packed)(lambda: unpack(i))
        for h in range(chunks[i][0], sum(chunks[i])):
            attn_n[h] = dot_nt(pick[...], attn[h]).astype(BF16)

    def issue(g):
        rightward(lambda: attn_copy(c, g, ar_s, c + 1, start, attn_hbm))
        leftward(lambda: attn_copy(c, g, al_s, c - 1, start, attn_hbm))

    def mix_all(g):
        for j in range(nt):
            mix(g, last_of[j])

    def add_all():
        for j in range(nt):
            add_direct(last_of[j])

    def mix(i, b):
        terms = None
        for h in range(chunks[i][0], sum(chunks[i])):
            g, r = h // repeat, h % repeat
            term = dot(attn_n[h], onehot[b]) * dot_nt(values[g], reads[b, g, :, r * hd:(r + 1) * hd])
            terms = term if terms is None else terms + term
        edges[b] = terms if i == 0 else edges[b] + terms

    def to_mate(b):
        for z in range(nx):
            send(edges.at[b, erow(z * 2 + 1 - core)], core_in.at[b, z], ce_s.at[0], ce_r.at[b], "src", mate)

    def over_x(b):
        arrived(core_in.at[b], ce_r.at[b])
        for dx in range(1, nx):
            z = lax.rem(x + dx, nx)
            x_out[b, z] = (edges[b, erow(z * 2 + core)] + core_in[b, z]).astype(BF16)
            send(x_out.at[b, z], x_in.at[b, x], xe_s.at[0], xe_r.at[b, dx - 1], "src", z * 2 + core)

    def over_z(b, away):
        mine = edges[b, erow(s)] + core_in[b, x]
        for dx in range(1, nx):
            z = lax.rem(x + dx, nx)
            arrived(x_in.at[b, z], xe_r.at[b, nx - 1 - dx])
            mine += x_in[b, z].astype(F32)
        if away:
            z_out[b] = mine.astype(BF16)
            send(z_out.at[b], z_in.at[c], ze_s.at[0], ze_r.at[0], "tgt", b)
        return mine

    spread(3)
    issue(0)
    take(1)
    issue(1)
    take(2)
    cross(0)
    issue(2)
    cross(1)
    value_step(1)
    ready(0)
    take(3)
    issue(3)
    ready(1)
    read_block(0, 1)
    read_block(1, 0)
    attn_step(1, 0)
    issue(4)
    read_block(0, 0)
    attn_step(1, 1)
    read_block(1, 1)
    attn_step(1, 2)
    value_step(2)
    attn_step(1, 3)
    cross(2)
    ready(2)
    attn_step(2, 0)
    read_block(2, 1)
    pl.when(jnp.logical_not(inner))(send_slices)
    pl.when(inner)(send_slices)
    cross(3)
    value_step(3)
    attn_step(2, 1)
    attn_step(1, 4)
    read_block(2, 0)
    ready(3)
    read_block(3, 1)
    attn_step(3, 0)
    pick_keys(0)
    read_block(3, 0)
    mix_all(0)
    attn_step(2, 2)
    attn_step(3, 1)
    pick_keys(1)
    attn_step(2, 3)
    mix_all(1)
    wait_slices()
    add_all()
    attn_step(3, 2)
    pick_keys(2)
    mix_all(2)
    attn_step(2, 4)
    attn_step(3, 3)
    pick_keys(3)
    mix_all(3)
    attn_step(3, 4)
    last = len(chunks) - 1
    pick_keys(last)
    mix(last, last_of[1])
    to_mate(last_of[1])
    mix(last, last_of[2])
    to_mate(last_of[2])
    for j in range(3, nt):
        mix(last, last_of[j])
        to_mate(last_of[j])
        over_x(last_of[j - 2])
    mix(last, c)
    to_mate(c)
    over_x(last_of[nt - 2])
    over_x(last_of[nt - 1])
    over_x(c)
    for j in range(1, nt):
        over_z(last_of[j], True)
    mine = over_z(c, False)
    fetch[8].wait()
    def drained(view, ssem):
        remote(view, view, ssem.at[0], local_sem.at[0], "src", mate).wait_send()

    drained(tslices.at[:nt - 1, :rows], zt_s)
    drained(tslices.at[:, :(nx - 1) * rows], xt_s)
    drained(tslices.at[:, :nx * rows], ct_s)
    drained(dslices.at[:(nt - 1) * sub], zd_s)
    drained(tpos.at[:nt - 1], zp_s)
    drained(decfull.at[:(nx - 1) * sub], xf_s)
    drained(decfull.at[:nx * sub], cf_s)
    drained(core_in, ce_s)
    drained(x_out.at[:, :nx - 1], xe_s)
    drained(z_out.at[:nt - 1], ze_s)

    def tiles(b):
        return heads if b < lowest else 3 * groups if b == packed else 2 * heads

    for i in range(nt):
        @pl.when(c == i)
        def _():
            if i + 1 < nt:
                drained(vproj.at[0, :queries * sum(tiles(b) for b in range(i + 1))], ar_s)
                drained(values.at[:, :(i + 1) * block], vr_s)
            if i > 0:
                drained(vproj.at[0, :queries * sum(tiles(b) for b in range(i, nt))], al_s)
                drained(values.at[:, :(nt - i) * block], vl_s)

    arrived(z_in.at[:nt - 1], ze_r.at[0])
    for j in range(1, nt):
        mine += z_in[order[j]].astype(F32)
    kept = pat_ref[(s * own) // block, c]
    out_ref[...] = (mine * kept.astype(F32)).astype(BF16)


def resident_shards(
    target_rows, target_pos, decoder_rows, source_pos, out_proj, value_proj, attention, tile_pattern
):
    nt, ns = lax.axis_size("tgt"), lax.axis_size("src")
    rows = target_rows.shape[0]
    sub, width = decoder_rows.shape
    heads, depth, head_dim = out_proj.shape
    groups = value_proj.shape[0]
    repeat = heads // groups
    _, queries, keys = attention.shape
    total = source_pos.shape[0]
    targets = target_pos.shape[0]
    own = total // ns
    nx = ns // 2
    vmem = pl.BlockSpec(memory_space=pltpu.VMEM)
    hbm = pl.BlockSpec(memory_space=pl.ANY)
    sem = lambda *shape: pltpu.SemaphoreType.DMA(shape)
    return pl.pallas_call(
        functools.partial(edge_kernel, nt, ns),
        out_shape=pltpu.VMEM((own, targets), BF16),
        in_specs=[hbm] * 8,
        out_specs=vmem,
        scratch_shapes=[
            pltpu.VMEM(out_proj.shape, BF16),
            pltpu.VMEM(value_proj.shape, BF16),
            pltpu.VMEM((nt, ns * rows, depth), BF16),
            pltpu.VMEM((nt * sub, depth), BF16),
            pltpu.VMEM((ns * sub, width), BF16),
            pltpu.VMEM((heads, nt * queries, keys), BF16),
            pltpu.VMEM((groups, 3, queries, keys // 2), BF16),
            pltpu.VMEM((nt, 1, targets), jnp.int32),
            pltpu.VMEM((1, total), jnp.int32),
            pltpu.VMEM((groups, total, head_dim), BF16),
            pltpu.VMEM((nt, groups, targets, repeat * head_dim), BF16),
            pltpu.VMEM((total, keys), BF16),
            pltpu.VMEM((heads, total, nt * queries), BF16),
            pltpu.VMEM((nt, nt * queries, targets), BF16),
            pltpu.VMEM((nt, total, targets), F32),
            pltpu.VMEM((nt, nx, own, targets), F32),
            pltpu.VMEM((nt, nx, own, targets), BF16),
            pltpu.VMEM((nt, nx, own, targets), BF16),
            pltpu.VMEM((nt, own, targets), BF16),
            pltpu.VMEM((nt, own, targets), BF16),
            pltpu.VMEM((total, 1), jnp.int32),
            pltpu.SMEM(tile_pattern.shape, jnp.int32),
            sem(10),
            sem(1), sem(nt), sem(1), sem(1), sem(1), sem(nt),
            sem(1), sem(1), sem(nt, groups + repeat - 1), sem(1), sem(1), sem(nt),
            sem(1), sem(nt, nx - 1), sem(1), sem(nt),
            sem(1), sem(nx - 1), sem(1), sem(1),
            sem(1), sem(nt), sem(1), sem(nt, nx - 1), sem(1), sem(1),
        ],
        compiler_params=pltpu.CompilerParams(
            collective_id=0, has_side_effects=True, vmem_limit_bytes=60 * 1024 * 1024
        ),
    )(
        target_rows, target_pos.reshape(1, targets), decoder_rows, source_pos.reshape(1, total),
        out_proj, value_proj, attention, tile_pattern,
    )


def resident_bytes(nt, ns, width, heads, depth, groups, rows, total, targets):
    weights = heads * depth * 128 + groups * width * 128
    gathered = nt * ns * rows * depth + nt * heads * targets * 128
    return 2 * (weights + gathered) + 4 * nt * total * targets * 2


def shards(
    target_rows, target_pos, decoder_rows, source_pos, out_proj, value_proj, attention, tile_pattern
):
    nt, ns = lax.axis_size("tgt"), lax.axis_size("src")
    heads, depth, head_dim = out_proj.shape
    need = resident_bytes(
        nt, ns, target_rows.shape[1], heads, depth, value_proj.shape[0], target_rows.shape[0],
        source_pos.shape[0], target_pos.shape[0],
    )
    fits = (
        depth % 128 == 0 and head_dim == 128 and ns % 2 == 0 and ns > 2 and nt > 2
        and decoder_rows.shape[0] % 16 == 0 and attention.shape[1] % 16 == 0
        and attention.shape[2] == 2 * head_dim and nt == 4
        and value_proj.shape[0] == 4 and heads == 8
        and 2 * heads * attention.shape[1] * nt <= target_rows.shape[1]
        and need < 40 * 1024 * 1024
    )
    plan = resident_shards if fits else gathered_shards
    return plan(
        target_rows, target_pos, decoder_rows, source_pos, out_proj, value_proj, attention, tile_pattern
    )


def solution(mesh):
    return jax.shard_map(
        shards,
        mesh=mesh,
        in_specs=(
            P(("grp", "tgt", "src"), None),
            P(("grp", "tgt")),
            P(("grp", "tgt", "src"), None),
            P("grp"),
            P("src", "tgt", None),
            P("src", None, None),
            P(("grp", "src"), "tgt", None),
            P("grp", None),
        ),
        out_specs=P(("grp", "src"), "tgt"),
        check_vma=False,
    )
```
